256 devices in a mesh: band: 32 (over y_hi, z, core), fft: 8 (over x, y_lo).
Axes of the slice: x: 4, y: 4 (y_hi: 2, y_lo: 2; y = y_hi * 2 + y_lo), z: 8, core: 2. Of those that a mesh axis runs over, the one named last changes fastest.
Arguments:
- coefficients: float32 [32, 2, 72, 5184], P('band', None, None, 'fft'), may hold values from -0.009765625 to 0.009765625
- col_index: int32 [5184], replicated, may hold values from 0 to 5183, each once
- occupation: int32 [32], P('band'), may hold values from 1 to 4
Outputs:
- density: float32 [288, 288, 288], P('band', 'fft')
The draws below stay inside these ranges and needn't reach their ends.
Inputs may be any that keep to these rules, and one draw needn't show every extreme that they name: `col_index`: each number of the range appears once.
All inputs are finite; a program needn't handle non-finite values.
Results may differ from the reference program's by a relative error of at most 0.0003.
Values sent between devices are 32-bit elements; how exact they have to be, the bound alone decides.
No kernel may reach another device: no remote copies, remote signals or barrier semaphores. Data moves between devices by JAX's collectives and lax.ppermute only.
A program may use at most 64 MiB of HBM per device.

```python
import jax
import jax.numpy as jnp
from jax import lax

NC = 144
NF = 288
KZ = 72
R = 36
NCOLS = 5184
BANDS = 32


def set_ends(values, rng, smallest, top_value):
    index_at = [jax.random.randint(jax.random.fold_in(rng, axis), (), 0, length) for axis, length in enumerate(values.shape)]
    widest = values.shape.index(max(values.shape))
    next_to = index_at[:widest] + [(index_at[widest] + 1) % values.shape[widest]] + index_at[widest + 1:]
    return values.at[tuple(index_at)].set(smallest).at[tuple(next_to)].set(top_value)


def block_levels(stream_key, extent, cuts, least, top_value):
    def one(dim, parts):
        steps = jax.random.uniform(jax.random.fold_in(jax.random.fold_in(stream_key, 6), dim), (parts,), jnp.float32, least / len(cuts), top_value / len(cuts))
        return jnp.repeat(jnp.exp(steps), extent[dim] // parts).reshape((-1,) + (1,) * (len(extent) - dim - 1))

    loudness = one(*cuts[0])
    for cut in cuts[1:]:
        loudness = loudness * one(*cut)
    return loudness


def noise(own_key, shape, scale, limit, shards=(), kind=jnp.bfloat16):
    entries = jax.random.normal(own_key, shape, jnp.float32) * scale
    if len(shards) > 0:
        entries = block_levels(own_key, shape, shards, -0.22, 0.18) * entries
    return jnp.clip(entries, min=-limit, max=limit).astype(kind)


def setup_inputs(seed: int = 0) -> dict:
    splits = jax.random.split(jax.random.key(seed), 4)
    return {
        "coefficients": noise(splits[0], (BANDS, 2, KZ, NCOLS), (8 * R**3) ** -0.5, 0.009765625, ((0, 32), (3, 8)), jnp.float32),
        "col_index": jax.random.permutation(splits[1], NCOLS).astype(jnp.int32),
        "occupation": set_ends(jax.random.randint(splits[2], (BANDS,), 1, 5), jax.random.fold_in(splits[2], 1), 1, 4).astype(jnp.int32),
    }


def sphere_mask(radius, side_len):
    wave_index = jnp.arange(side_len, dtype=jnp.int32) - radius
    square = wave_index * wave_index
    total_sq = square[:, None, None] + square[None, :, None] + square[None, None, :]
    return (total_sq <= radius * radius).astype(jnp.float32)


def reference(coefficients, col_index, occupation):
    inverse = jnp.zeros((NCOLS,), jnp.int32).at[col_index].set(jnp.arange(NCOLS, dtype=jnp.int32))
    inside = sphere_mask(R, KZ)

    def add_band(band_index, summed):
        box_grid = jnp.take(coefficients[band_index], inverse, axis=2).reshape(2, KZ, KZ, KZ)
        box_grid = jnp.transpose(box_grid, (0, 2, 3, 1)) * inside
        spectrum = lax.complex(box_grid[0], box_grid[1])
        padded = jnp.zeros((NC, NC, NC), spectrum.dtype).at[:KZ, :KZ, :KZ].set(spectrum)
        padded = jnp.roll(padded, (-R, -R, -R), axis=(0, 1, 2))
        wave_field = jnp.fft.ifftn(padded) * float(NC * NC * NC)
        real_part = jnp.real(wave_field)
        imag_part = jnp.imag(wave_field)
        moduli = real_part * real_part + imag_part * imag_part
        return summed + occupation[band_index].astype(jnp.float32) * moduli

    coarse_density = lax.fori_loop(0, BANDS, add_band, jnp.zeros((NC, NC, NC), jnp.float32)) / BANDS
    spectrum = jnp.fft.fftn(coarse_density) / float(NC * NC * NC)
    kept_mask = (jnp.arange(NC, dtype=jnp.int32) != NC // 2).astype(jnp.float32)
    spectrum = spectrum * (kept_mask[:, None, None] * kept_mask[None, :, None] * kept_mask[None, None, :])
    target = jnp.arange(NC, dtype=jnp.int32)
    target = jnp.where(target < NC // 2, target, target + NF - NC)
    fine_spec = jnp.zeros((NF, NF, NF), spectrum.dtype)
    fine_spec = fine_spec.at[target[:, None, None], target[None, :, None], target[None, None, :]].set(spectrum)
    density = jnp.real(jnp.fft.ifftn(fine_spec)) * float(NF * NF * NF)
    return density.astype(jnp.float32)
```

```python
import jax
import jax.numpy as jnp
import ml_dtypes
import numpy as np
from jax import lax
from jax.experimental import pallas as pl
from jax.experimental.pallas import tpu as pltpu
from jax.sharding import Mesh, PartitionSpec as P

NC = 144
NF = 288
KZ = 72
NCOLS = 5184
BANDS = 32
R2 = (KZ // 2) ** 2

AXES = ("yh", "z", "core", "x", "yl")
SIZES = (2, 8, 2, 4, 2)
PLANE = ("yh", "x", "yl")
NP = NC // 16
CB = NCOLS // 8
GR = 96
NG = 7
R2ROWS = 200
R3ROWS = 32

F32 = jnp.float32
BF16 = jnp.bfloat16


def split_np(table):
    hi = table.astype(np.float32).astype(ml_dtypes.bfloat16)
    lo = (table - hi.astype(np.float64)).astype(np.float32).astype(ml_dtypes.bfloat16)
    return hi, lo


def wave_tables():
    k = np.arange(KZ) - KZ // 2
    phase = np.mod(k[:, None] * np.arange(NC)[None, :], NC) * (2 * np.pi / NC)
    return np.cos(phase), np.sin(phase)


def interpolation_np():
    offset = np.arange(NF)[:, None] - 2 * np.arange(NC)[None, :]
    k = np.arange(1, NC // 2)
    phase = np.mod(offset[:, :, None] * k, NF) * (2 * np.pi / NF)
    return (1 + 2 * np.cos(phase).sum(2)) / NC


def tables():
    c, s = wave_tables()
    u = interpolation_np()
    w1 = np.zeros((2 * KZ, 384))
    for q in range(16):
        t, v = divmod(q, NG)
        at = 128 * t + 9 * v
        pl_ = slice(NP * q, NP * q + NP)
        w1[:KZ, at : at + NP] = c[:, pl_]
        w1[KZ:, at : at + NP] = -s[:, pl_]
        w1[:KZ, at + 64 : at + 64 + NP] = s[:, pl_]
        w1[KZ:, at + 64 : at + 64 + NP] = c[:, pl_]
    e2 = np.zeros((256, 512))
    e2[:KZ, :NC] = c
    e2[128 : 128 + KZ, :NC] = -s
    e2[:KZ, 256 : 256 + NC] = s
    e2[128 : 128 + KZ, 256 : 256 + NC] = c
    er = np.concatenate([np.concatenate([c.T, -s.T], 1), np.concatenate([s.T, c.T], 1)], 0)
    rows = np.array(
        [
            [9 * (16 * yh + 2 * z + core) + g for z in range(8) for yh in range(2) for g in range(9)]
            for core in range(2)
        ]
    )
    ug = u[rows]
    uf = np.zeros((NC, 384))
    for fb in range(8):
        t, v = divmod(fb, 3)
        uf[:, 128 * t + 36 * v : 128 * t + 36 * v + 36] = u[36 * fb : 36 * fb + 36].T
    uft = np.tile(uf[128:], (8, 1))
    return w1, e2, er, ug, uf[:128], uft, u.T


def fold(table, axis):
    hi, lo = split_np(table)
    return np.concatenate([hi, hi, lo], axis)


def split(x):
    hi = x.astype(BF16)
    return hi, (x - hi.astype(F32)).astype(BF16)


def dot(a, b):
    return jnp.dot(a, b, preferred_element_type=F32)


def dot3(a, b_hi, b_lo):
    hi, lo = split(a)
    return dot(hi, b_hi) + (dot(hi, b_lo) + dot(lo, b_hi))


def lanes(shape):
    return lax.broadcasted_iota(jnp.int32, shape, 1)


def k1_body(occ_ref, x_ref, col_ref, whi_ref, wlo_ref, o_ref, xs, ys):
    fft = lax.axis_index("x") * 2 + lax.axis_index("yl")
    col = col_ref[pl.ds(fft, 1), :]
    k0 = jnp.floor((col.astype(F32) + 0.5) * (1.0 / KZ)).astype(jnp.int32)
    k1 = col - k0 * KZ - KZ // 2
    k0 = k0 - KZ // 2
    k2 = lax.broadcasted_iota(jnp.int32, (KZ, CB), 0) - KZ // 2
    inside = k2 * k2 + (k0 * k0 + k1 * k1) <= R2
    xs[:, 640:768] = jnp.zeros((2 * KZ, 128), F32)
    xs[0:KZ, 0:CB] = jnp.where(inside, x_ref[0, 0], 0.0)
    xs[KZ : 2 * KZ, 0:CB] = jnp.where(inside, x_ref[0, 1], 0.0)
    for j in range(6):
        rows = 128 if j < 5 else 32
        xt = xs[:, 128 * j : 128 * j + 128].T[0:rows]
        ys[128 * j : 128 * j + rows, :] = dot3(xt, whi_ref[...], wlo_ref[...])
    weight = occ_ref[0].astype(F32) * (1.0 / BANDS)
    lane = lanes((GR, 128))
    for q in range(16):
        t, v = divmod(q, NG)
        acc = jnp.full((GR, 128), weight, F32)
        for g in range(NG):
            part = ys[GR * g : GR * g + GR, 128 * t : 128 * t + 128]
            if g != v:
                part = pltpu.roll(part, (9 * (g - v)) % 128, 1)
            half = lane & 63
            acc = jnp.where((half >= 9 * g) & (half < 9 * g + 9), part, acc)
        o_ref[q] = acc


def k2_body(row_ref, r_ref, ehi_ref, elo_ref, er_ref, ug_ref, keep_ref, send_ref, st, box, hs, gs):
    core = lax.axis_index("core")
    box[...] = jnp.zeros(box.shape, F32)
    lane = lanes((GR, 128)) & 63
    for fb in range(8):
        for g in range(NG):
            n = min(GR, CB - GR * g)
            first = r_ref[fb, 0:n, :]
            second = r_ref[8 + fb, 0:n, :]
            if g != 0:
                first = pltpu.roll(first, (-9 * g) % 128, 1)
            if g != 1:
                second = pltpu.roll(second, (9 - 9 * g) % 128, 1)
            st[CB * fb + GR * g : CB * fb + GR * g + n, :] = jnp.where(lane[0:n] < 9, first, second)

    def place(i, carry):
        for t in range(16):
            c = i * 16 + t
            box[pl.ds(row_ref[c], 1), :] = st[pl.ds(c, 1), :]
        return carry

    lax.fori_loop(0, NCOLS // 16, place, 0)

    def along_second(i, carry):
        parts = []
        for t in range(8):
            at = pl.multiple_of((i * 8 + t) * 128, 128)
            flipped = box[pl.ds(at, 128), :].T
            parts.append(jnp.concatenate([flipped[0:24], flipped[64:88]], 1))
        line = jnp.concatenate(parts, 0)
        half = dot3(line, ehi_ref[...], elo_ref[...])
        for j in range(4):
            hs[j, pl.ds(pl.multiple_of(i * 192, 192), 192), :] = half[:, 128 * j : 128 * j + 128]
        return carry

    lax.fori_loop(0, 9, along_second, 0)

    def plane(p, carry):
        density = None
        for b in range(2):
            half = [hs[j, pl.ds(9 * b + p, KZ, stride=24), :] for j in range(4)]
            rows = [jnp.concatenate(half[0:2], 1), jnp.concatenate(half[2:4], 1)]
            hi, lo = split(jnp.concatenate(rows, 0))
            full = dot(er_ref[...], jnp.concatenate([hi, lo, hi], 0))
            sq = full * full
            part = (sq[0:NC] + sq[NC : 2 * NC]) * r_ref[8 * b, 0:1, 63:64]
            density = part if density is None else density + part
        hi, lo = split(density)
        rhs = jnp.concatenate([hi, lo, hi], 0)
        gs[p, 0:NC, :] = dot(ug_ref[core], rhs)
        gs[p, NC : 2 * NC, :] = dot(ug_ref[1 - core], rhs)
        return carry

    lax.fori_loop(0, NP, plane, 0)
    tail_lane = lanes((18, 128))
    for part, out in enumerate((keep_ref, send_ref)):
        for z in range(8):
            at = NC * part + 18 * z
            tail = None
            for p in range(NP):
                out[z, 18 * p : 18 * p + 18, :] = gs[p, at : at + 18, 0:128]
                end = gs[p, at : at + 18, 128:256]
                if p == 8:
                    out[z, 180:198, :] = end
                elif p == 0:
                    tail = end
                else:
                    tail = jnp.where(tail_lane < 16 * p, tail, pltpu.roll(end, 16 * p, 1))
            out[z, 162:180, :] = tail


def k3_body(r_ref, fhi_ref, flo_ref, thi_ref, tlo_ref, o_ref, ss, ts, fs):
    total = r_ref[0]
    for z in range(1, 8):
        total = total + r_ref[z]
    ss[...] = total
    lane = lanes((18, 128))
    ts[160:168, :] = jnp.zeros((8, 128), F32)
    for p in range(NP):
        if p < 8:
            tail = jnp.where((lane >= 16 * p) & (lane < 16 * p + 16), ss[162:180, :], 0.0)
        else:
            tail = jnp.where(lane < 16, ss[180:198, :], 0.0)
        ts[18 * p : 18 * p + 18, :] = tail
    fine = dot3(ss[0:168, :], fhi_ref[...], flo_ref[...]) + dot3(
        ts[...], thi_ref[...], tlo_ref[...]
    )
    for t in range(3):
        fs[t] = fine[:, 128 * t : 128 * t + 128]
    lane = lanes((NP, 128))
    for yh in range(2):
        for fb in range(8):
            t, v = divmod(fb, 3)
            for b in range(3):
                acc = None
                for a in range(3):
                    part = fs[t, pl.ds(9 * yh + 3 * a + b, NP, stride=18), :]
                    if a != v:
                        part = pltpu.roll(part, (36 * (a - v)) % 128, 1)
                    acc = part if acc is None else jnp.where(lane < 36 * a, acc, part)
                o_ref[8 * yh + fb, 9 * b : 9 * b + 9, :] = acc


def k4_body(r_ref, uhi_ref, ulo_ref, o_ref, xs, ys):
    for b in range(3):
        for q in range(16):
            xs[b, 9 * q : 9 * q + 9, :] = r_ref[q, 9 * b : 9 * b + 9, :]
        ys[b] = dot3(xs[b].T, uhi_ref[...], ulo_ref[...])
        for a in range(3):
            o_ref[3 * a + b] = ys[b, 36 * a : 36 * a + 36, :]


def vmem(n):
    return [pl.BlockSpec(memory_space=pltpu.VMEM)] * n


def smem():
    return [pl.BlockSpec(memory_space=pltpu.SMEM)]


def call(body, name, in_specs, outs, scratch, flops):
    return pl.pallas_call(
        body,
        out_shape=outs,
        in_specs=in_specs,
        out_specs=jax.tree.map(lambda _: pl.BlockSpec(memory_space=pltpu.VMEM), outs),
        scratch_shapes=[pltpu.VMEM(s, F32) for s in scratch],
        name=name,
        cost_estimate=pl.CostEstimate(flops=flops, bytes_accessed=2_000_000, transcendentals=0),
    )


def shape(*dims):
    return jax.ShapeDtypeStruct(dims, F32)


def local(coefficients, col_index, occupation):
    w1, e2, er, ug, uf, uft, uh = tables()
    whi, wlo = split_np(w1)
    ehi, elo = split_np(e2)
    fhi, flo = split_np(uf)
    thi, tlo = split_np(uft)
    uhi, ulo = split_np(uh)
    columns = col_index.reshape(8, CB)
    rows = (col_index // KZ) * 128 + col_index % KZ
    sent = call(
        k1_body, "lines", smem() + vmem(4), shape(16, GR, 128), [(2 * KZ, 768), (NG * GR, 384)], 10**9
    )(occupation, coefficients, columns, whi, wlo)
    got = lax.all_to_all(sent, PLANE, split_axis=0, concat_axis=0, tiled=True)
    keep, send = call(
        k2_body,
        "planes",
        smem() + vmem(5),
        (shape(8, R2ROWS, 128), shape(8, R2ROWS, 128)),
        [(NCOLS, 128), (KZ * 128, 128), (4, KZ * 24, 128), (NP, NF, 256)],
        10**10,
    )(rows, got, ehi, elo, fold(er, 1), fold(ug, 2))
    keep = keep + lax.ppermute(send, "core", [(0, 1), (1, 0)])
    got = lax.all_to_all(keep, "z", split_axis=0, concat_axis=0, tiled=True)
    sent = call(
        k3_body,
        "second",
        vmem(5),
        shape(16, R3ROWS, 128),
        [(R2ROWS, 128), (168, 128), (3, 168, 128)],
        10**9,
    )(got, fhi, flo, thi, tlo)
    got = lax.all_to_all(sent, PLANE, split_axis=0, concat_axis=0, tiled=True)
    return call(
        k4_body, "third", vmem(3), shape(9, 36, NF), [(3, NC, 128), (3, 128, NF)], 10**9
    )(got, uhi, ulo)


def solution(mesh):
    axes = Mesh(mesh.devices.reshape(SIZES), AXES)
    band, fft = ("yh", "z", "core"), ("x", "yl")
    return jax.shard_map(
        local,
        mesh=axes,
        in_specs=(P(band, None, None, fft), P(), P(band)),
        out_specs=P(band, fft, None),
        check_vma=False,
    )
```

```python
import jax
import jax.numpy as jnp
import ml_dtypes
import numpy as np
from jax import lax
from jax.experimental import pallas as pl
from jax.experimental.pallas import tpu as pltpu
from jax.sharding import Mesh, PartitionSpec as P

NC = 144
NF = 288
KZ = 72
NCOLS = 5184
BANDS = 32
R2 = (KZ // 2) ** 2

AXES = ("yh", "zh", "zl", "core", "x", "yl")
SIZES = (2, 4, 2, 2, 4, 2)
BAND, FFT = ("yh", "zh", "zl", "core"), ("x", "yl")
PLANE = ("yh", "x", "yl", "zl")
ND = 32
NB = 4
NP = 5
NZ = ND * NP
CB = NCOLS // 8
GR = 56
NG = 12
R2ROWS = 216
R3ROWS = 16

F32 = jnp.float32
BF16 = jnp.bfloat16


def split_np(table):
    hi = table.astype(np.float32).astype(ml_dtypes.bfloat16)
    lo = (table - hi.astype(np.float64)).astype(np.float32).astype(ml_dtypes.bfloat16)
    return hi, lo


def wave_tables(points):
    k = np.arange(KZ) - KZ // 2
    phase = np.mod(k[:, None] * np.arange(points)[None, :], points) * (2 * np.pi / points)
    return np.cos(phase), np.sin(phase)


def interpolation_np(points):
    offset = np.arange(NF)[:, None] * points - NF * np.arange(points)[None, :]
    k = np.arange(1, NC // 2)
    phase = np.mod(offset[:, :, None] * k, NF * points) * (2 * np.pi / (NF * points))
    return (1 + 2 * np.cos(phase).sum(2)) / points


def tables():
    c, s = wave_tables(NZ)
    w1 = np.zeros((2 * KZ, 384))
    for q in range(ND):
        t, v = divmod(q, NG)
        at = 128 * t + NP * v
        own = slice(NP * q, NP * q + NP)
        w1[:KZ, at : at + NP] = c[:, own]
        w1[KZ:, at : at + NP] = -s[:, own]
        w1[:KZ, at + 64 : at + 64 + NP] = s[:, own]
        w1[KZ:, at + 64 : at + 64 + NP] = c[:, own]
    c, s = wave_tables(NC)
    e2 = np.zeros((256, 512))
    e2[:KZ, :NC] = c
    e2[128 : 128 + KZ, :NC] = -s
    e2[:KZ, 256 : 256 + NC] = s
    e2[128 : 128 + KZ, 256 : 256 + NC] = c
    er = np.concatenate([np.concatenate([c.T, -s.T], 1), np.concatenate([s.T, c.T], 1)], 0)
    u = interpolation_np(NC)
    rows = np.array(
        [
            [9 * (16 * yh + 2 * z + core) + g for z in range(8) for yh in range(2) for g in range(9)]
            for core in range(2)
        ]
    )
    ug = u[rows]
    uf = np.zeros((NC, 384))
    for fb in range(8):
        t, v = divmod(fb, 3)
        uf[:, 128 * t + 36 * v : 128 * t + 36 * v + 36] = u[36 * fb : 36 * fb + 36].T
    uft = np.tile(uf[128:], (8, 1))
    return w1, e2, er, ug, uf[:128], uft, interpolation_np(NZ).T


def fold(table, axis):
    hi, lo = split_np(table)
    return np.concatenate([hi, hi, lo], axis)


def split(x):
    hi = x.astype(BF16)
    return hi, (x - hi.astype(F32)).astype(BF16)


def dot(a, b):
    return jnp.dot(a, b, preferred_element_type=F32)


def dot3(a, b_hi, b_lo):
    hi, lo = split(a)
    return dot(hi, b_hi) + (dot(hi, b_lo) + dot(lo, b_hi))


def lanes(shape):
    return lax.broadcasted_iota(jnp.int32, shape, 1)


def k1_body(occ_ref, x_ref, col_ref, whi_ref, wlo_ref, o_ref, xs, ys):
    fft = lax.axis_index("x") * 2 + lax.axis_index("yl")
    col = col_ref[pl.ds(fft, 1), :]
    k0 = jnp.floor((col.astype(F32) + 0.5) * (1.0 / KZ)).astype(jnp.int32)
    k1 = col - k0 * KZ - KZ // 2
    k0 = k0 - KZ // 2
    k2 = lax.broadcasted_iota(jnp.int32, (KZ, CB), 0) - KZ // 2
    inside = k2 * k2 + (k0 * k0 + k1 * k1) <= R2
    xs[:, 640:768] = jnp.zeros((2 * KZ, 128), F32)
    xs[0:KZ, 0:CB] = jnp.where(inside, x_ref[0, 0], 0.0)
    xs[KZ : 2 * KZ, 0:CB] = jnp.where(inside, x_ref[0, 1], 0.0)
    for j in range(6):
        rows = 128 if j < 5 else 32
        xt = xs[:, 128 * j : 128 * j + 128].T[0:rows]
        ys[128 * j : 128 * j + rows, :] = dot3(xt, whi_ref[...], wlo_ref[...])
    weight = occ_ref[0].astype(F32) * (1.0 / BANDS)
    lane = lanes((GR, 128))
    for q in range(ND):
        t, v = divmod(q, NG)
        acc = jnp.full((GR, 128), weight, F32)
        for g in range(NG):
            part = ys[GR * g : GR * g + GR, 128 * t : 128 * t + 128]
            if g != v:
                part = pltpu.roll(part, (NP * (g - v)) % 128, 1)
            half = lane & 63
            acc = jnp.where((half >= NP * g) & (half < NP * g + NP), part, acc)
        o_ref[q] = acc


def k2_body(row_ref, r_ref, ehi_ref, elo_ref, er_ref, ug_ref, keep_ref, send_ref, st, box, hs, gs):
    core = lax.axis_index("core")
    box[...] = jnp.zeros(box.shape, F32)
    lane = lanes((GR, 128)) & 63
    for fb in range(8):
        for g in range(NG):
            n = min(GR, CB - GR * g)
            acc = None
            for b in range(NB):
                part = r_ref[source(b, fb), 0:n, :]
                if b != g:
                    part = pltpu.roll(part, (NP * (b - g)) % 128, 1)
                acc = part if acc is None else jnp.where(lane[0:n] < NP * b, acc, part)
            st[CB * fb + GR * g : CB * fb + GR * g + n, :] = acc

    def place(i, carry):
        for t in range(48):
            c = i * 48 + t
            box[pl.ds(row_ref[c], 1), :] = st[pl.ds(c, 1), :]
        return carry

    lax.fori_loop(0, NCOLS // 48, place, 0)

    def along_second(i, carry):
        parts = []
        for t in range(8):
            at = pl.multiple_of((i * 8 + t) * 128, 128)
            flipped = box[pl.ds(at, 128), :].T
            parts.append(jnp.concatenate([flipped[0:24], flipped[64:88]], 1))
        line = jnp.concatenate(parts, 0)
        half = dot3(line, ehi_ref[...], elo_ref[...])
        for j in range(4):
            hs[j, pl.ds(pl.multiple_of(i * 192, 192), 192), :] = half[:, 128 * j : 128 * j + 128]
        return carry

    lax.fori_loop(0, 9, along_second, 0)

    def plane(p, carry):
        density = None
        for b in range(NB):
            half = [hs[j, pl.ds(NP * b + p, KZ, stride=24), :] for j in range(4)]
            rows = [jnp.concatenate(half[0:2], 1), jnp.concatenate(half[2:4], 1)]
            hi, lo = split(jnp.concatenate(rows, 0))
            full = dot(er_ref[...], jnp.concatenate([hi, lo, hi], 0))
            sq = full * full
            part = (sq[0:NC] + sq[NC : 2 * NC]) * r_ref[source(b, 0), 0:1, 63:64]
            density = part if density is None else density + part
        hi, lo = split(density)
        rhs = jnp.concatenate([hi, lo, hi], 0)
        gs[p, 0:NC, :] = dot(ug_ref[core], rhs)
        gs[p, NC : 2 * NC, :] = dot(ug_ref[1 - core], rhs)
        return carry

    lax.fori_loop(0, NP, plane, 0)
    tail_lane = lanes((36, 128))
    for part, out in enumerate((keep_ref, send_ref)):
        for z in range(4):
            at = NC * part + 36 * z
            tail = None
            for p in range(NP):
                out[z, 36 * p : 36 * p + 36, :] = gs[p, at : at + 36, 0:128]
                end = gs[p, at : at + 36, 128:256]
                if p == 0:
                    tail = end
                else:
                    tail = jnp.where(tail_lane < 16 * p, tail, pltpu.roll(end, 16 * p, 1))
            out[z, 36 * NP : 36 * NP + 36, :] = tail


def source(b, fb):
    return 16 * (b // 2) + 2 * fb + b % 2


def k3_body(r_ref, fhi_ref, flo_ref, thi_ref, tlo_ref, o_ref, ss, ts, fs):
    ss[...] = (r_ref[0] + r_ref[1]) + (r_ref[2] + r_ref[3])
    lane = lanes((36, 128))
    ts[176:184, :] = jnp.zeros((8, 128), F32)
    for p in range(NP):
        own = (lane >= 16 * p) & (lane < 16 * p + 16)
        ts[36 * p : 36 * p + 36, :] = jnp.where(own, ss[36 * NP : 36 * NP + 36, :], 0.0)
    fine = dot3(ss[0:184, :], fhi_ref[...], flo_ref[...]) + dot3(
        ts[...], thi_ref[...], tlo_ref[...]
    )
    for t in range(3):
        fs[t] = fine[:, 128 * t : 128 * t + 128]
    lane = lanes((NP, 128))
    for yh in range(2):
        for zl in range(2):
            for fb in range(8):
                t, v = divmod(fb, 3)
                for b in range(3):
                    acc = None
                    for a in range(3):
                        first = 18 * zl + 9 * yh + 3 * a + b
                        part = fs[t, pl.ds(first, NP, stride=36), :]
                        if a != v:
                            part = pltpu.roll(part, (36 * (a - v)) % 128, 1)
                        acc = part if acc is None else jnp.where(lane < 36 * a, acc, part)
                    o_ref[16 * yh + 2 * fb + zl, NP * b : NP * b + NP, :] = acc


def k4_body(r_ref, uhi_ref, ulo_ref, o_ref, xs, ys):
    for b in range(3):
        for q in range(ND):
            xs[b, NP * q : NP * q + NP, :] = r_ref[q, NP * b : NP * b + NP, :]
        ys[b] = dot3(xs[b].T, uhi_ref[...], ulo_ref[...])
        for a in range(3):
            o_ref[3 * a + b] = ys[b, 36 * a : 36 * a + 36, :]


def vmem(n):
    return [pl.BlockSpec(memory_space=pltpu.VMEM)] * n


def smem():
    return [pl.BlockSpec(memory_space=pltpu.SMEM)]


def call(body, name, in_specs, outs, scratch, flops, mib=12):
    return pl.pallas_call(
        body,
        out_shape=outs,
        in_specs=in_specs,
        out_specs=jax.tree.map(lambda _: pl.BlockSpec(memory_space=pltpu.VMEM), outs),
        scratch_shapes=[pltpu.VMEM(s, F32) for s in scratch],
        name=name,
        compiler_params=pltpu.CompilerParams(vmem_limit_bytes=mib * 2**20),
        cost_estimate=pl.CostEstimate(flops=flops, bytes_accessed=2_000_000, transcendentals=0),
    )


def shape(*dims):
    return jax.ShapeDtypeStruct(dims, F32)


def local(coefficients, col_index, occupation):
    w1, e2, er, ug, uf, uft, uh = tables()
    whi, wlo = split_np(w1)
    ehi, elo = split_np(e2)
    fhi, flo = split_np(uf)
    thi, tlo = split_np(uft)
    uhi, ulo = split_np(uh)
    columns = col_index.reshape(8, CB)
    rows = (col_index // KZ) * 128 + col_index % KZ
    sent = call(
        k1_body, "lines", smem() + vmem(4), shape(ND, GR, 128), [(2 * KZ, 768), (NG * GR, 384)], 10**9
    )(occupation, coefficients, columns, whi, wlo)
    got = lax.all_to_all(sent, PLANE, split_axis=0, concat_axis=0, tiled=True)
    keep, send = call(
        k2_body,
        "planes",
        smem() + vmem(5),
        (shape(4, R2ROWS, 128), shape(4, R2ROWS, 128)),
        [(NCOLS, 128), (KZ * 128, 128), (4, KZ * 24, 128), (NP, NF, 256)],
        10**10,
        28,
    )(rows, got, ehi, elo, fold(er, 1), fold(ug, 2))
    keep = keep + lax.ppermute(send, "core", [(0, 1), (1, 0)])
    got = lax.all_to_all(keep, "zh", split_axis=0, concat_axis=0, tiled=True)
    sent = call(
        k3_body,
        "second",
        vmem(5),
        shape(ND, R3ROWS, 128),
        [(R2ROWS, 128), (184, 128), (3, 184, 128)],
        10**9,
    )(got, fhi, flo, thi, tlo)
    got = lax.all_to_all(sent, PLANE, split_axis=0, concat_axis=0, tiled=True)
    return call(
        k4_body, "third", vmem(3), shape(9, 36, NF), [(3, NZ, 128), (3, 128, NF)], 10**9
    )(got, uhi, ulo)


def solution(mesh):
    axes = Mesh(mesh.devices.reshape(SIZES), AXES)
    return jax.shard_map(
        local,
        mesh=axes,
        in_specs=(P(BAND, None, None, FFT), P(), P(BAND)),
        out_specs=P(BAND, FFT, None),
        check_vma=False,
    )
```

```python
import jax
import jax.numpy as jnp
import ml_dtypes
import numpy as np
from jax import lax
from jax.experimental import pallas as pl
from jax.experimental.pallas import tpu as pltpu
from jax.sharding import Mesh, PartitionSpec as P

NC = 144
NF = 288
KZ = 72
NCOLS = 5184
BANDS = 32
R2 = (KZ // 2) ** 2

AXES = ("yh", "zh", "zl", "core", "x", "yl")
SIZES = (2, 4, 2, 2, 4, 2)
BAND, FFT = ("yh", "zh", "zl", "core"), ("x", "yl")
PLANE = ("yh", "x", "yl", "zl")
ND = 32
NB = 4
NP = 5
NZ = ND * NP
CB = NCOLS // 8
R1ROWS = 56
R2ROWS = 216
R3ROWS = 16

F32 = jnp.float32
BF16 = jnp.bfloat16


def split_np(table):
    hi = table.astype(np.float32).astype(ml_dtypes.bfloat16)
    lo = (table - hi.astype(np.float64)).astype(np.float32).astype(ml_dtypes.bfloat16)
    return hi, lo


def wave_tables(points):
    k = np.arange(KZ) - KZ // 2
    phase = np.mod(k[:, None] * np.arange(points)[None, :], points) * (2 * np.pi / points)
    return np.cos(phase), np.sin(phase)


def interpolation_np(points):
    offset = np.arange(NF)[:, None] * points - NF * np.arange(points)[None, :]
    k = np.arange(1, NC // 2)
    phase = np.mod(offset[:, :, None] * k, NF * points) * (2 * np.pi / (NF * points))
    return (1 + 2 * np.cos(phase).sum(2)) / points


def tables():
    c, s = wave_tables(NZ)
    w1 = np.concatenate([np.concatenate([c.T, -s.T], 1), np.concatenate([s.T, c.T], 1)], 0)
    c, s = wave_tables(NC)
    e2 = np.zeros((256, 512))
    e2[:KZ, :NC] = c
    e2[128 : 128 + KZ, :NC] = -s
    e2[:KZ, 256 : 256 + NC] = s
    e2[128 : 128 + KZ, 256 : 256 + NC] = c
    er = np.concatenate([np.concatenate([c.T, -s.T], 1), np.concatenate([s.T, c.T], 1)], 0)
    u = interpolation_np(NC)
    ug = np.zeros((2, 4, 40, NC))
    for core in range(2):
        for z in range(8):
            for yh in range(2):
                at = 18 * (z % 2) + 9 * yh
                first = 9 * (16 * yh + 2 * z + core)
                ug[core, z // 2, at : at + 9] = u[first : first + 9]
    ug = ug.reshape(2, 160, NC)
    uf = np.zeros((NC, 384))
    for fb in range(8):
        t, v = divmod(fb, 3)
        uf[:, 128 * t + 36 * v : 128 * t + 36 * v + 36] = u[36 * fb : 36 * fb + 36].T
    uft = np.tile(uf[128:], (8, 1))
    return w1, e2, er, ug, uf[:128], uft, interpolation_np(NZ).T


def fold(table, axis):
    hi, lo = split_np(table)
    return np.concatenate([hi, hi, lo], axis)


def split(x):
    hi = x.astype(BF16)
    return hi, (x - hi.astype(F32)).astype(BF16)


def dot(a, b):
    return jnp.dot(a, b, preferred_element_type=F32)


def dot3(a, b_hi, b_lo):
    hi, lo = split(a)
    return dot(hi, b_hi) + (dot(hi, b_lo) + dot(lo, b_hi))


def lanes(shape):
    return lax.broadcasted_iota(jnp.int32, shape, 1)


def k1_body(occ_hbm, x_hbm, col_ref, w_hbm, o_ref, occ_ref, xr, wv, xs, ys, sems):
    copies = [
        pltpu.make_async_copy(occ_hbm, occ_ref, sems.at[0]),
        pltpu.make_async_copy(x_hbm.at[0], xr, sems.at[1]),
        pltpu.make_async_copy(w_hbm, wv, sems.at[2]),
    ]
    for copy in copies:
        copy.start()
    fft = lax.axis_index("x") * 2 + lax.axis_index("yl")
    col = col_ref[pl.ds(fft, 1), :]
    k0 = jnp.floor((col.astype(F32) + 0.5) * (1.0 / KZ)).astype(jnp.int32)
    k1 = col - k0 * KZ - KZ // 2
    k0 = k0 - KZ // 2
    k2 = lax.broadcasted_iota(jnp.int32, (KZ, CB), 0) - KZ // 2
    inside = k2 * k2 + (k0 * k0 + k1 * k1) <= R2
    xs[:, 640:768] = jnp.zeros((2 * KZ, 128), F32)
    for copy in copies:
        copy.wait()
    xs[0:KZ, 0:CB] = jnp.where(inside, xr[0], 0.0)
    xs[KZ : 2 * KZ, 0:CB] = jnp.where(inside, xr[1], 0.0)
    for n in range(3):
        hi, lo = split(xs[:, 256 * n : 256 * n + 256])
        y = dot(wv[...], jnp.concatenate([hi, lo, hi], 0))
        ys[2 * n] = y[:, 0:128]
        ys[2 * n + 1] = y[:, 128:256]
    lane = lanes((NZ, 128))
    ys[5, 0:NZ, :] = jnp.where(lane < 8, ys[5, 0:NZ, :], pltpu.roll(ys[5, NZ : 2 * NZ, :], 8, 1))
    weight = jnp.full((1, 128), occ_ref[0].astype(F32) * (1.0 / BANDS), F32)
    for q in range(ND):
        for j in range(6):
            for ri in range(2 if j < 5 else 1):
                at, own = 10 * j + NP * ri, NZ * ri + NP * q
                o_ref[q, at : at + NP, :] = ys[j, own : own + NP, :]
        o_ref[q, 55:56, :] = weight


def source(b, fb):
    return 16 * (b // 2) + 2 * fb + b % 2


def k2_body(row_ref, r_ref, ehi_ref, elo_ref, er_ref, ug_ref, *rest):
    keep2, keep0, keep1, keep3, send2, send_rest, tr, st, box, hs, gs = rest
    core = lax.axis_index("core")
    zh = lax.axis_index("zh")
    box[NCOLS : NCOLS + 56, :] = jnp.zeros((56, 128), F32)

    def unpack(fb, carry):
        base = pl.multiple_of(fb * CB, 8)
        for j in range(6):
            for b in range(NB):
                for ri in range(2 if j < 5 else 1):
                    at = 24 * ri + NP * b
                    own = 10 * j + NP * ri
                    tr[j, at : at + NP, :] = r_ref[source(b, fb), own : own + NP, :]
            if j < 5:
                st[pl.ds(pl.multiple_of(base + 128 * j, 8), 128), 0:48] = tr[j].T
            else:
                tr[5, 24:48, :] = pltpu.roll(tr[5, 0:24, :], 120, 1)
                st[pl.ds(pl.multiple_of(base + 640, 8), 8), 0:48] = tr[5].T[0:8]
        return carry

    lax.fori_loop(0, 8, unpack, 0)

    def place(i, carry):
        for t in range(48):
            c = i * 48 + t
            box[pl.ds(row_ref[c], 1), :] = st[pl.ds(c, 1), :]
        return carry

    lax.fori_loop(0, NCOLS // 48, place, 0)

    def along_second(i, carry):
        parts = []
        for t in range(8):
            at = pl.multiple_of((i * 8 + t) * KZ, 8)
            flipped = box[pl.ds(at, 128), :].T
            parts.append(jnp.concatenate([flipped[0:24], flipped[24:48]], 1))
        line = jnp.concatenate(parts, 0)
        half = dot3(line, ehi_ref[...], elo_ref[...])
        for j in range(4):
            hs[j, pl.ds(pl.multiple_of(i * 192, 192), 192), :] = half[:, 128 * j : 128 * j + 128]
        return carry

    lax.fori_loop(0, 9, along_second, 0)

    def plane(p, carry):
        density = None
        for b in range(NB):
            half = [hs[j, pl.ds(NP * b + p, KZ, stride=24), :] for j in range(4)]
            rows = [jnp.concatenate(half[0:2], 1), jnp.concatenate(half[2:4], 1)]
            hi, lo = split(jnp.concatenate(rows, 0))
            full = dot(er_ref[...], jnp.concatenate([hi, lo, hi], 0))
            sq = full * full
            part = (sq[0:NC] + sq[NC : 2 * NC]) * r_ref[source(b, 0), 55:56, 0:1]
            density = part if density is None else density + part
        hi, lo = split(density)
        rhs = jnp.concatenate([hi, lo, hi], 0)
        gs[p, 0] = dot(ug_ref[core], rhs).reshape(4, 40, 256)
        gs[p, 1] = dot(ug_ref[1 - core], rhs).reshape(4, 40, 256)
        return carry

    lax.fori_loop(0, NP, plane, 0)
    tail_lane = lanes((36, 128))
    sends = [send_rest.at[0], send_rest.at[1], send2, send_rest.at[2]]
    for part, outs in enumerate(((keep0, keep1, keep2, keep3), sends)):
        for d in range(4):
            z = (zh + d) & 3
            tail = None
            for p in range(NP):
                outs[d][36 * p : 36 * p + 36, :] = gs[p, part, z, 0:36, 0:128]
                end = gs[p, part, z, 0:36, 128:256]
                if p == 0:
                    tail = end
                else:
                    tail = jnp.where(tail_lane < 16 * p, tail, pltpu.roll(end, 16 * p, 1))
            outs[d][36 * NP : 36 * NP + 36, :] = tail


def k3_body(r0_ref, r1_ref, r2_ref, fhi_ref, flo_ref, thi_ref, tlo_ref, o_ref, ss, ts, fs):
    ss[...] = r0_ref[...] + (r1_ref[...] + r2_ref[...])
    lane = lanes((36, 128))
    ts[176:184, :] = jnp.zeros((8, 128), F32)
    for p in range(NP):
        own = (lane >= 16 * p) & (lane < 16 * p + 16)
        ts[36 * p : 36 * p + 36, :] = jnp.where(own, ss[36 * NP : 36 * NP + 36, :], 0.0)
    fine = dot3(ss[0:184, :], fhi_ref[...], flo_ref[...]) + dot3(
        ts[...], thi_ref[...], tlo_ref[...]
    )
    for t in range(3):
        fs[t] = fine[:, 128 * t : 128 * t + 128]
    lane = lanes((NP, 128))
    for yh in range(2):
        for zl in range(2):
            for fb in range(8):
                t, v = divmod(fb, 3)
                for b in range(3):
                    acc = None
                    for a in range(3):
                        first = 18 * zl + 9 * yh + 3 * a + b
                        part = fs[t, pl.ds(first, NP, stride=36), :]
                        if a != v:
                            part = pltpu.roll(part, (36 * (a - v)) % 128, 1)
                        acc = part if acc is None else jnp.where(lane < 36 * a, acc, part)
                    o_ref[16 * yh + 2 * fb + zl, NP * b : NP * b + NP, :] = acc


def k4_body(r_ref, uhi_ref, ulo_ref, o_ref, xs, ys):
    for b in range(3):
        for q in range(ND):
            xs[b, NP * q : NP * q + NP, :] = r_ref[q, NP * b : NP * b + NP, :]
        ys[b] = dot3(xs[b].T, uhi_ref[...], ulo_ref[...])
        for a in range(3):
            o_ref[3 * a + b] = ys[b, 36 * a : 36 * a + 36, :]


def vmem(n):
    return [pl.BlockSpec(memory_space=pltpu.VMEM)] * n


def smem():
    return [pl.BlockSpec(memory_space=pltpu.SMEM)]


def call(body, name, in_specs, outs, scratch, flops, mib=12):
    return pl.pallas_call(
        body,
        out_shape=outs,
        in_specs=in_specs,
        out_specs=jax.tree.map(lambda _: pl.BlockSpec(memory_space=pltpu.VMEM), outs),
        scratch_shapes=[pltpu.VMEM(s, F32) if isinstance(s, tuple) else s for s in scratch],
        name=name,
        compiler_params=pltpu.CompilerParams(vmem_limit_bytes=mib * 2**20),
        cost_estimate=pl.CostEstimate(flops=flops, bytes_accessed=2_000_000, transcendentals=0),
    )


def shape(*dims):
    return jax.ShapeDtypeStruct(dims, F32)


def local(coefficients, col_index, occupation):
    w1, e2, er, ug, uf, uft, uh = tables()
    ehi, elo = split_np(e2)
    fhi, flo = split_np(uf)
    thi, tlo = split_np(uft)
    uhi, ulo = split_np(uh)
    columns = col_index.reshape(8, CB)
    hbm = pl.BlockSpec(memory_space=pltpu.HBM)
    sent = call(
        k1_body,
        "lines",
        [hbm, hbm] + vmem(1) + [hbm],
        shape(ND, R1ROWS, 128),
        [
            pltpu.SMEM((1,), jnp.int32),
            (2, KZ, CB),
            pltpu.VMEM((2 * NZ, 6 * KZ), BF16),
            (2 * KZ, 768),
            (6, 2 * NZ, 128),
            pltpu.SemaphoreType.DMA((3,)),
        ],
        10**9,
    )(occupation, coefficients, columns, fold(w1, 1))
    got = lax.all_to_all(sent, PLANE, split_axis=0, concat_axis=0, tiled=True)
    block = shape(R2ROWS, 128)
    keep2, keep0, keep1, keep3, send2, send_rest = call(
        k2_body,
        "planes",
        smem() + vmem(5),
        (block, block, block, block, block, shape(3, R2ROWS, 128)),
        [
            (6, 48, 128),
            (NCOLS, 128),
            (NCOLS + 56, 128),
            (4, KZ * 24, 128),
            (NP, 2, 4, 40, 256),
        ],
        10**10,
        24,
    )(col_index, got, ehi, elo, fold(er, 1), fold(ug, 2))
    swap = [(0, 1), (1, 0)]
    up = [(i, (i + 1) % 4) for i in range(4)]
    down = [(i, (i - 1) % 4) for i in range(4)]
    keep2 = keep2 + lax.ppermute(send2, "core", swap)
    rest = lax.ppermute(send_rest, "core", swap)
    from_below = lax.ppermute(keep2[:104], "zh", up)
    from_above = lax.ppermute(keep2[104:], "zh", down)
    keep1 = keep1 + rest[1]
    keep3 = keep3 + rest[2]
    keep1 = jnp.concatenate([keep1[:104] + from_below, keep1[104:]], 0)
    keep3 = jnp.concatenate([keep3[:104], keep3[104:] + from_above], 0)
    from_below = lax.ppermute(keep1, "zh", up)
    from_above = lax.ppermute(keep3, "zh", down)
    sent = call(
        k3_body,
        "second",
        vmem(7),
        shape(ND, R3ROWS, 128),
        [(R2ROWS, 128), (184, 128), (3, 184, 128)],
        10**9,
    )(keep0 + rest[0], from_below, from_above, fhi, flo, thi, tlo)
    got = lax.all_to_all(sent, PLANE, split_axis=0, concat_axis=0, tiled=True)
    return call(
        k4_body, "third", vmem(3), shape(9, 36, NF), [(3, NZ, 128), (3, 128, NF)], 10**9
    )(got, uhi, ulo)


def solution(mesh):
    axes = Mesh(mesh.devices.reshape(SIZES), AXES)
    return jax.shard_map(
        local,
        mesh=axes,
        in_specs=(P(BAND, None, None, FFT), P(), P(BAND)),
        out_specs=P(BAND, FFT, None),
        check_vma=False,
    )
```

```python
import jax
import jax.numpy as jnp
import ml_dtypes
import numpy as np
from jax import lax
from jax.experimental import pallas as pl
from jax.experimental.pallas import tpu as pltpu
from jax.sharding import Mesh, PartitionSpec as P

NC = 144
NF = 288
KZ = 72
NCOLS = 5184
BANDS = 32
R2 = (KZ // 2) ** 2

AXES = ("yh", "zh", "zl", "core", "x", "yl")
SIZES = (2, 4, 2, 2, 4, 2)
BAND, FFT = ("yh", "zh", "zl", "core"), ("x", "yl")
PLANE = ("yh", "x", "yl", "zl")
ND = 32
NB = 4
NP = 5
NZ = ND * NP
CB = NCOLS // 8
R1ROWS = 56
R2ROWS = 216
R3ROWS = 16

F32 = jnp.float32
BF16 = jnp.bfloat16


def split_np(table):
    hi = table.astype(np.float32).astype(ml_dtypes.bfloat16)
    lo = (table - hi.astype(np.float64)).astype(np.float32).astype(ml_dtypes.bfloat16)
    return hi, lo


def wave_tables(points):
    k = np.arange(KZ) - KZ // 2
    phase = np.mod(k[:, None] * np.arange(points)[None, :], points) * (2 * np.pi / points)
    return np.cos(phase), np.sin(phase)


def interpolation_np(points):
    offset = np.arange(NF)[:, None] * points - NF * np.arange(points)[None, :]
    k = np.arange(1, NC // 2)
    phase = np.mod(offset[:, :, None] * k, NF * points) * (2 * np.pi / (NF * points))
    return (1 + 2 * np.cos(phase).sum(2)) / points


def tables():
    c, s = wave_tables(NZ)
    w1 = np.concatenate([np.concatenate([c.T, -s.T], 1), np.concatenate([s.T, c.T], 1)], 0)
    c, s = wave_tables(NC)
    e2 = np.zeros((256, 384))
    for ri, (on_re, on_im) in enumerate(((c, -s), (s, c))):
        for at, own in ((128 * ri, slice(0, 128)), (256 + 16 * ri, slice(128, NC))):
            width = own.stop - own.start
            e2[:KZ, at : at + width] = on_re[:, own]
            e2[128 : 128 + KZ, at : at + width] = on_im[:, own]
    er = np.concatenate([np.concatenate([c.T, -s.T], 1), np.concatenate([s.T, c.T], 1)], 0)
    u = interpolation_np(NC)
    ug = np.zeros((2, 4, 40, NC))
    for core in range(2):
        for z in range(8):
            for yh in range(2):
                at = 18 * (z % 2) + 9 * yh
                first = 9 * (16 * yh + 2 * z + core)
                ug[core, z // 2, at : at + 9] = u[first : first + 9]
    ug = ug.reshape(2, 160, NC)
    uf = np.zeros((NC, 384))
    for fb in range(8):
        t, v = divmod(fb, 3)
        uf[:, 128 * t + 36 * v : 128 * t + 36 * v + 36] = u[36 * fb : 36 * fb + 36].T
    uft = np.tile(uf[128:], (8, 1))
    return w1, e2, er, ug, uf[:128], uft, interpolation_np(NZ).T


def fold(table, axis):
    hi, lo = split_np(table)
    return np.concatenate([hi, hi, lo], axis)


def split(x):
    hi = x.astype(BF16)
    return hi, (x - hi.astype(F32)).astype(BF16)


def dot(a, b):
    return jnp.dot(a, b, preferred_element_type=F32)


def dot3(a, b_hi, b_lo):
    hi, lo = split(a)
    return dot(hi, b_hi) + (dot(hi, b_lo) + dot(lo, b_hi))


def lanes(shape):
    return lax.broadcasted_iota(jnp.int32, shape, 1)


def k1_body(occ_ref, x_ref, w_ref, o_ref, ys):
    for n in range(3):
        hi, lo = split(x_ref[:, 256 * n : 256 * n + 256])
        y = dot(w_ref[...], jnp.concatenate([hi, lo, hi], 0))
        ys[2 * n] = y[:, 0:128]
        ys[2 * n + 1] = y[:, 128:256]
    lane = lanes((NZ, 128))
    ys[5, 0:NZ, :] = jnp.where(lane < 8, ys[5, 0:NZ, :], pltpu.roll(ys[5, NZ : 2 * NZ, :], 8, 1))
    weight = jnp.full((1, 128), occ_ref[0].astype(F32) * (1.0 / BANDS), F32)
    for q in range(ND):
        for j in range(6):
            for ri in range(2 if j < 5 else 1):
                at, own = 10 * j + NP * ri, NZ * ri + NP * q
                o_ref[q, at : at + NP, :] = ys[j, own : own + NP, :]
        o_ref[q, 55:56, :] = weight


def source(b, fb):
    return 16 * (b // 2) + 2 * fb + b % 2


def k2_body(row_ref, r_ref, ehi_ref, elo_ref, er_ref, ug_ref, *rest):
    keep2, keep0, keep1, keep3, send2, send_rest, tr, st, box, hs, gs, col_ref, sem = rest
    columns = pltpu.make_async_copy(row_ref, col_ref, sem)
    columns.start()
    core = lax.axis_index("core")
    zh = lax.axis_index("zh")
    box[NCOLS : NCOLS + 56, :] = jnp.zeros((56, 128), F32)

    def unpack(fb, carry):
        base = fb * CB
        for j in range(6):
            for b in range(NB):
                for ri in range(2 if j < 5 else 1):
                    at = 24 * ri + NP * b
                    own = 10 * j + NP * ri
                    tr[6 * fb + j, at : at + NP, :] = r_ref[source(b, fb), own : own + NP, :]
            if j < 5:
                st[pl.ds(base + 128 * j, 128), 0:48] = tr[6 * fb + j].T
            else:
                tr[6 * fb + 5, 24:48, :] = pltpu.roll(tr[6 * fb + 5, 0:24, :], 120, 1)
                st[pl.ds(base + 640, 8), 0:48] = tr[6 * fb + 5].T[0:8]
        return carry

    for fb in range(8):
        unpack(fb, 0)
    columns.wait()

    def place(i, carry):
        for t in range(216):
            c = i * 216 + t
            box[pl.ds(col_ref[c], 1), :] = st[pl.ds(c, 1), :]
        return carry

    lax.fori_loop(0, NCOLS // 216, place, 0)

    def along_second(i, carry):
        parts = []
        for t in range(36):
            at = pl.multiple_of((i * 36 + t) * KZ, 8)
            flipped = box[pl.ds(at, 128), :].T
            parts.append(jnp.concatenate([flipped[0:24], flipped[24:48]], 1))
        line = jnp.concatenate(parts, 0)
        half = dot3(line, ehi_ref[...], elo_ref[...])
        for j in range(3):
            hs[j, pl.ds(pl.multiple_of(i * 864, 8), 864), :] = half[:, 128 * j : 128 * j + 128]
        return carry

    lax.fori_loop(0, 2, along_second, 0)

    lane = lanes((NC, 128))

    def transformed(field):
        hi, lo = split(field)
        full = dot(er_ref[...], jnp.concatenate([hi, lo, hi], 0))
        sq = full * full
        return sq[0:NC] + sq[NC : 2 * NC]

    def plane(p, carry):
        weight = [r_ref[source(b, 0), 55:56, 0:1] for b in range(NB)]
        mains, tail, factor = [], None, None
        for b in range(NB):
            re, im, end = [hs[j, pl.ds(NP * b + p, KZ, stride=24), :] for j in range(3)]
            mains.append(jnp.concatenate([re, im], 0))
            re = pltpu.roll(end, 16 * b, 1) if b else end
            im = pltpu.roll(end, 16 * b - 16, 1) if b > 1 else end if b else pltpu.roll(end, 112, 1)
            end = jnp.concatenate([re, im], 0)
            tail = jnp.where(lane < 16 * b, tail, end) if b else end
            factor = jnp.where(lane < 16 * b, factor, weight[b]) if b else weight[b]
        density = None
        for b in range(0, NB, 2):
            pair = transformed(jnp.concatenate(mains[b : b + 2], 1))
            pair = pair[:, 0:128] * weight[b] + pair[:, 128:256] * weight[b + 1]
            density = pair if density is None else density + pair
        tail = transformed(tail) * factor
        tail = tail + pltpu.roll(tail, 96, 1)
        tail = tail + pltpu.roll(tail, 112, 1)
        density = jnp.concatenate([density, tail], 1)
        hi, lo = split(density)
        rhs = jnp.concatenate([hi, lo, hi], 0)
        gs[p, 0] = dot(ug_ref[core], rhs).reshape(4, 40, 256)
        gs[p, 1] = dot(ug_ref[1 - core], rhs).reshape(4, 40, 256)
        return carry

    for p in range(NP):
        plane(p, 0)
    tail_lane = lanes((36, 128))
    sends = [send_rest.at[0], send_rest.at[1], send2, send_rest.at[2]]
    for part, outs in enumerate(((keep0, keep1, keep2, keep3), sends)):
        for d in range(4):
            z = (zh + d) & 3
            tail = None
            for p in range(NP):
                outs[d][36 * p : 36 * p + 36, :] = gs[p, part, z, 0:36, 0:128]
                end = gs[p, part, z, 0:36, 128:256]
                if p == 0:
                    tail = end
                else:
                    tail = jnp.where(tail_lane < 16 * p, tail, pltpu.roll(end, 16 * p, 1))
            outs[d][36 * NP : 36 * NP + 36, :] = tail


def k3_body(r0_ref, r1_ref, r2_ref, fhi_ref, flo_ref, thi_ref, tlo_ref, o_ref, ss, ts, fs):
    ss[...] = r0_ref[...] + (r1_ref[...] + r2_ref[...])
    lane = lanes((36, 128))
    ts[176:184, :] = jnp.zeros((8, 128), F32)
    for p in range(NP):
        own = (lane >= 16 * p) & (lane < 16 * p + 16)
        ts[36 * p : 36 * p + 36, :] = jnp.where(own, ss[36 * NP : 36 * NP + 36, :], 0.0)
    fine = dot3(ss[0:184, :], fhi_ref[...], flo_ref[...]) + dot3(
        ts[...], thi_ref[...], tlo_ref[...]
    )
    for t in range(3):
        fs[t] = fine[:, 128 * t : 128 * t + 128]
    lane = lanes((NP, 128))
    for yh in range(2):
        for zl in range(2):
            for fb in range(8):
                t, v = divmod(fb, 3)
                for b in range(3):
                    acc = None
                    for a in range(3):
                        first = 18 * zl + 9 * yh + 3 * a + b
                        part = fs[t, pl.ds(first, NP, stride=36), :]
                        if a != v:
                            part = pltpu.roll(part, (36 * (a - v)) % 128, 1)
                        acc = part if acc is None else jnp.where(lane < 36 * a, acc, part)
                    o_ref[16 * yh + 2 * fb + zl, NP * b : NP * b + NP, :] = acc


def k4_body(r_ref, uhi_ref, ulo_ref, o_ref, xs, ys):
    for b in range(3):
        for q in range(ND):
            xs[b, NP * q : NP * q + NP, :] = r_ref[q, NP * b : NP * b + NP, :]
        ys[b] = dot3(xs[b].T, uhi_ref[...], ulo_ref[...])
        for a in range(3):
            o_ref[3 * a + b] = ys[b, 36 * a : 36 * a + 36, :]


def vmem(n):
    return [pl.BlockSpec(memory_space=pltpu.VMEM)] * n


def smem():
    return [pl.BlockSpec(memory_space=pltpu.SMEM)]


def call(body, name, in_specs, outs, scratch, flops, mib=12):
    return pl.pallas_call(
        body,
        out_shape=outs,
        in_specs=in_specs,
        out_specs=jax.tree.map(lambda _: pl.BlockSpec(memory_space=pltpu.VMEM), outs),
        scratch_shapes=[pltpu.VMEM(s, F32) if isinstance(s, tuple) else s for s in scratch],
        name=name,
        compiler_params=pltpu.CompilerParams(vmem_limit_bytes=mib * 2**20),
        cost_estimate=pl.CostEstimate(flops=flops, bytes_accessed=2_000_000, transcendentals=0),
    )


def shape(*dims):
    return jax.ShapeDtypeStruct(dims, F32)


def local(coefficients, col_index, occupation):
    w1, e2, er, ug, uf, uft, uh = tables()
    ehi, elo = split_np(e2)
    fhi, flo = split_np(uf)
    thi, tlo = split_np(uft)
    uhi, ulo = split_np(uh)
    fft = lax.axis_index("x") * 2 + lax.axis_index("yl")
    columns = lax.dynamic_slice_in_dim(col_index, fft * CB, CB)
    k0 = columns // KZ - KZ // 2
    k1 = columns % KZ - KZ // 2
    k2 = jnp.arange(KZ, dtype=jnp.int32) - KZ // 2
    inside = (k0 * k0 + k1 * k1)[None, :] + (k2 * k2)[:, None] <= R2
    masked = jnp.where(inside, coefficients[0], 0.0).reshape(2 * KZ, CB)
    masked = jnp.pad(masked, ((0, 0), (0, 768 - CB)))
    sent = call(
        k1_body,
        "lines",
        smem() + vmem(2),
        shape(ND, R1ROWS, 128),
        [(6, 2 * NZ, 128)],
        10**9,
    )(occupation, masked, fold(w1, 1))
    got = lax.all_to_all(sent, PLANE, split_axis=0, concat_axis=0, tiled=True)
    block = shape(R2ROWS, 128)
    keep2, keep0, keep1, keep3, send2, send_rest = call(
        k2_body,
        "planes",
        [pl.BlockSpec(memory_space=pl.ANY)] + vmem(5),
        (block, block, block, block, block, shape(3, R2ROWS, 128)),
        [
            (48, 48, 128),
            (NCOLS, 128),
            (NCOLS + 56, 128),
            (3, KZ * 24, 128),
            (NP, 2, 4, 40, 256),
            pltpu.SMEM((NCOLS,), jnp.int32),
            pltpu.SemaphoreType.DMA,
        ],
        10**10,
        24,
    )(col_index, got, ehi, elo, fold(er, 1), fold(ug, 2))
    swap = [(0, 1), (1, 0)]
    up = [(i, (i + 1) % 4) for i in range(4)]
    down = [(i, (i - 1) % 4) for i in range(4)]
    keep2 = keep2 + lax.ppermute(send2, "core", swap)
    rest = lax.ppermute(send_rest, "core", swap)
    from_below = lax.ppermute(keep2[:104], "zh", up)
    from_above = lax.ppermute(keep2[104:], "zh", down)
    keep1 = keep1 + rest[1]
    keep3 = keep3 + rest[2]
    keep1 = jnp.concatenate([keep1[:104] + from_below, keep1[104:]], 0)
    keep3 = jnp.concatenate([keep3[:104], keep3[104:] + from_above], 0)
    from_below = lax.ppermute(keep1, "zh", up)
    from_above = lax.ppermute(keep3, "zh", down)
    sent = call(
        k3_body,
        "second",
        vmem(7),
        shape(ND, R3ROWS, 128),
        [(R2ROWS, 128), (184, 128), (3, 184, 128)],
        10**9,
    )(keep0 + rest[0], from_below, from_above, fhi, flo, thi, tlo)
    got = lax.all_to_all(sent, PLANE, split_axis=0, concat_axis=0, tiled=True)
    return call(
        k4_body, "third", vmem(3), shape(9, 36, NF), [(3, NZ, 128), (3, 128, NF)], 10**9
    )(got, uhi, ulo)


def solution(mesh):
    axes = Mesh(mesh.devices.reshape(SIZES), AXES)
    return jax.shard_map(
        local,
        mesh=axes,
        in_specs=(P(BAND, None, None, FFT), P(), P(BAND)),
        out_specs=P(BAND, FFT, None),
        check_vma=False,
    )
```

```python
import jax
import jax.numpy as jnp
import ml_dtypes
import numpy as np
from jax import lax
from jax.experimental import pallas as pl
from jax.experimental.pallas import tpu as pltpu
from jax.sharding import Mesh, PartitionSpec as P

NC = 144
NF = 288
KZ = 72
NCOLS = 5184
BANDS = 32
R2 = (KZ // 2) ** 2

AXES = ("yh", "zh", "zl", "core", "x", "yl")
SIZES = (2, 4, 2, 2, 4, 2)
BAND, FFT = ("yh", "zh", "zl", "core"), ("x", "yl")
PLANE = ("yh", "x", "yl", "zl")
ND = 32
NB = 4
NP = 5
NZ = ND * NP
CB = NCOLS // 8
R1ROWS = 56
R2ROWS = 216
R3ROWS = 16

F32 = jnp.float32
BF16 = jnp.bfloat16


def split_np(table):
    hi = table.astype(np.float32).astype(ml_dtypes.bfloat16)
    lo = (table - hi.astype(np.float64)).astype(np.float32).astype(ml_dtypes.bfloat16)
    return hi, lo


def wave_tables(points):
    k = np.arange(KZ) - KZ // 2
    phase = np.mod(k[:, None] * np.arange(points)[None, :], points) * (2 * np.pi / points)
    return np.cos(phase), np.sin(phase)


def interpolation_np(points):
    offset = np.arange(NF)[:, None] * points - NF * np.arange(points)[None, :]
    k = np.arange(1, NC // 2)
    phase = np.mod(offset[:, :, None] * k, NF * points) * (2 * np.pi / (NF * points))
    return (1 + 2 * np.cos(phase).sum(2)) / points


def tables():
    c, s = wave_tables(NZ)
    w1 = np.concatenate([np.concatenate([c.T, -s.T], 1), np.concatenate([s.T, c.T], 1)], 0)
    c, s = wave_tables(NC)
    e2 = np.zeros((256, 384))
    for ri, (on_re, on_im) in enumerate(((c, -s), (s, c))):
        for at, own in ((128 * ri, slice(0, 128)), (256 + 16 * ri, slice(128, NC))):
            width = own.stop - own.start
            e2[:KZ, at : at + width] = on_re[:, own]
            e2[128 : 128 + KZ, at : at + width] = on_im[:, own]
    er = np.concatenate([np.concatenate([c.T, -s.T], 1), np.concatenate([s.T, c.T], 1)], 0)
    u = interpolation_np(NC)
    ug = np.zeros((2, 4, 40, NC))
    for core in range(2):
        for z in range(8):
            for yh in range(2):
                at = 18 * (z % 2) + 9 * yh
                first = 9 * (16 * yh + 2 * z + core)
                ug[core, z // 2, at : at + 9] = u[first : first + 9]
    ug = ug.reshape(2, 160, NC)
    uf = np.zeros((NC, 384))
    for fb in range(8):
        t, v = divmod(fb, 3)
        uf[:, 128 * t + 36 * v : 128 * t + 36 * v + 36] = u[36 * fb : 36 * fb + 36].T
    uft = np.tile(uf[128:], (8, 1))
    return w1, e2, er, ug, uf[:128], uft, interpolation_np(NZ).T


def fold(table, axis):
    hi, lo = split_np(table)
    return np.concatenate([hi, hi, lo], axis)


def split(x):
    hi = x.astype(BF16)
    return hi, (x - hi.astype(F32)).astype(BF16)


def dot(a, b):
    return jnp.dot(a, b, preferred_element_type=F32)


def dot3(a, b_hi, b_lo):
    hi, lo = split(a)
    return dot(hi, b_hi) + (dot(hi, b_lo) + dot(lo, b_hi))


def lanes(shape):
    return lax.broadcasted_iota(jnp.int32, shape, 1)


def k1_body(occ_ref, x_ref, w_ref, o_ref, ys):
    for n in range(3):
        hi, lo = split(x_ref[:, 256 * n : 256 * n + 256])
        y = dot(w_ref[...], jnp.concatenate([hi, lo, hi], 0))
        ys[2 * n] = y[:, 0:128]
        ys[2 * n + 1] = y[:, 128:256]
    lane = lanes((NZ, 128))
    ys[5, 0:NZ, :] = jnp.where(lane < 8, ys[5, 0:NZ, :], pltpu.roll(ys[5, NZ : 2 * NZ, :], 8, 1))
    weight = jnp.full((1, 128), occ_ref[0].astype(F32) * (1.0 / BANDS), F32)
    for q in range(ND):
        for j in range(6):
            for ri in range(2 if j < 5 else 1):
                at, own = 10 * j + NP * ri, NZ * ri + NP * q
                o_ref[q, at : at + NP, :] = ys[j, own : own + NP, :]
        o_ref[q, 55:56, :] = weight


def source(b, fb):
    return 16 * (b // 2) + 2 * fb + b % 2


def k2_body(row_ref, r_ref, ehi_ref, elo_ref, er_ref, ug_ref, *rest):
    keep2, keep0, keep1, keep3, send2, send_rest, tr, st, box, hs, gs, col_ref, sem = rest
    columns = pltpu.make_async_copy(row_ref, col_ref, sem)
    columns.start()
    core = lax.axis_index("core")
    zh = lax.axis_index("zh")
    box[NCOLS : NCOLS + 56, :] = jnp.zeros((56, 128), F32)

    def unpack(fb, carry):
        base = fb * CB
        for j in range(6):
            for b in range(NB):
                for ri in range(2 if j < 5 else 1):
                    at = 24 * ri + NP * b
                    own = 10 * j + NP * ri
                    tr[6 * fb + j, at : at + NP, :] = r_ref[source(b, fb), own : own + NP, :]
            if j < 5:
                st[pl.ds(base + 128 * j, 128), 0:48] = tr[6 * fb + j].T
            else:
                tr[6 * fb + 5, 24:48, :] = pltpu.roll(tr[6 * fb + 5, 0:24, :], 120, 1)
                st[pl.ds(base + 640, 8), 0:48] = tr[6 * fb + 5].T[0:8]
        return carry

    for fb in range(8):
        unpack(fb, 0)
    columns.wait()

    views = [col_ref.at[pl.ds(t, NCOLS - 432 + 1)] for t in range(432)]

    def place(i, carry):
        at = i * 432
        for t in range(432):
            box[pl.ds(views[t][at], 1), :] = st[pl.ds(at + t, 1), :]
        return carry

    lax.fori_loop(0, NCOLS // 432, place, 0)

    def along_second(i, carry):
        parts = []
        for t in range(36):
            at = pl.multiple_of((i * 36 + t) * KZ, 8)
            flipped = box[pl.ds(at, 128), :].T
            parts.append(jnp.concatenate([flipped[0:24], flipped[24:48]], 1))
        line = jnp.concatenate(parts, 0)
        half = dot3(line, ehi_ref[...], elo_ref[...])
        for j in range(3):
            hs[j, pl.ds(pl.multiple_of(i * 864, 8), 864), :] = half[:, 128 * j : 128 * j + 128]
        return carry

    lax.fori_loop(0, 2, along_second, 0)

    lane = lanes((NC, 128))

    def transformed(field):
        hi, lo = split(field)
        full = dot(er_ref[...], jnp.concatenate([hi, lo, hi], 0))
        sq = full * full
        return sq[0:NC] + sq[NC : 2 * NC]

    def plane(p, carry):
        weight = [r_ref[source(b, 0), 55:56, 0:1] for b in range(NB)]
        mains, tail, factor = [], None, None
        for b in range(NB):
            re, im, end = [hs[j, pl.ds(NP * b + p, KZ, stride=24), :] for j in range(3)]
            mains.append(jnp.concatenate([re, im], 0))
            re = pltpu.roll(end, 16 * b, 1) if b else end
            im = pltpu.roll(end, 16 * b - 16, 1) if b > 1 else end if b else pltpu.roll(end, 112, 1)
            end = jnp.concatenate([re, im], 0)
            tail = jnp.where(lane < 16 * b, tail, end) if b else end
            factor = jnp.where(lane < 16 * b, factor, weight[b]) if b else weight[b]
        density = None
        for b in range(0, NB, 2):
            pair = transformed(jnp.concatenate(mains[b : b + 2], 1))
            pair = pair[:, 0:128] * weight[b] + pair[:, 128:256] * weight[b + 1]
            density = pair if density is None else density + pair
        tail = transformed(tail) * factor
        tail = tail + pltpu.roll(tail, 96, 1)
        tail = tail + pltpu.roll(tail, 112, 1)
        density = jnp.concatenate([density, tail], 1)
        hi, lo = split(density)
        rhs = jnp.concatenate([hi, lo, hi], 0)
        gs[p, 0] = dot(ug_ref[core], rhs).reshape(4, 40, 256)
        gs[p, 1] = dot(ug_ref[1 - core], rhs).reshape(4, 40, 256)
        return carry

    for p in range(NP):
        plane(p, 0)
    tail_lane = lanes((36, 128))
    sends = [send_rest.at[0], send_rest.at[1], send2, send_rest.at[2]]
    for part, outs in enumerate(((keep0, keep1, keep2, keep3), sends)):
        for d in range(4):
            z = (zh + d) & 3
            tail = None
            for p in range(NP):
                outs[d][36 * p : 36 * p + 36, :] = gs[p, part, z, 0:36, 0:128]
                end = gs[p, part, z, 0:36, 128:256]
                if p == 0:
                    tail = end
                else:
                    tail = jnp.where(tail_lane < 16 * p, tail, pltpu.roll(end, 16 * p, 1))
            outs[d][36 * NP : 36 * NP + 36, :] = tail


def k3_body(r0_ref, r1_ref, r2_ref, fhi_ref, flo_ref, thi_ref, tlo_ref, o_ref, ss, ts, fs):
    ss[...] = r0_ref[...] + (r1_ref[...] + r2_ref[...])
    lane = lanes((36, 128))
    ts[176:184, :] = jnp.zeros((8, 128), F32)
    for p in range(NP):
        own = (lane >= 16 * p) & (lane < 16 * p + 16)
        ts[36 * p : 36 * p + 36, :] = jnp.where(own, ss[36 * NP : 36 * NP + 36, :], 0.0)
    fine = dot3(ss[0:184, :], fhi_ref[...], flo_ref[...]) + dot3(
        ts[...], thi_ref[...], tlo_ref[...]
    )
    for t in range(3):
        fs[t] = fine[:, 128 * t : 128 * t + 128]
    lane = lanes((NP, 128))
    for yh in range(2):
        for zl in range(2):
            for fb in range(8):
                t, v = divmod(fb, 3)
                for b in range(3):
                    acc = None
                    for a in range(3):
                        first = 18 * zl + 9 * yh + 3 * a + b
                        part = fs[t, pl.ds(first, NP, stride=36), :]
                        if a != v:
                            part = pltpu.roll(part, (36 * (a - v)) % 128, 1)
                        acc = part if acc is None else jnp.where(lane < 36 * a, acc, part)
                    o_ref[16 * yh + 2 * fb + zl, NP * b : NP * b + NP, :] = acc


def k4_body(r_ref, uhi_ref, ulo_ref, o_ref, xs, ys):
    for b in range(3):
        for q in range(ND):
            xs[b, NP * q : NP * q + NP, :] = r_ref[q, NP * b : NP * b + NP, :]
        ys[b] = dot3(xs[b].T, uhi_ref[...], ulo_ref[...])
        for a in range(3):
            o_ref[3 * a + b] = ys[b, 36 * a : 36 * a + 36, :]


def vmem(n):
    return [pl.BlockSpec(memory_space=pltpu.VMEM)] * n


def smem():
    return [pl.BlockSpec(memory_space=pltpu.SMEM)]


def call(body, name, in_specs, outs, scratch, flops, mib=12):
    return pl.pallas_call(
        body,
        out_shape=outs,
        in_specs=in_specs,
        out_specs=jax.tree.map(lambda _: pl.BlockSpec(memory_space=pltpu.VMEM), outs),
        scratch_shapes=[pltpu.VMEM(s, F32) if isinstance(s, tuple) else s for s in scratch],
        name=name,
        compiler_params=pltpu.CompilerParams(vmem_limit_bytes=mib * 2**20),
        cost_estimate=pl.CostEstimate(flops=flops, bytes_accessed=2_000_000, transcendentals=0),
    )


def shape(*dims):
    return jax.ShapeDtypeStruct(dims, F32)


def local(coefficients, col_index, occupation):
    w1, e2, er, ug, uf, uft, uh = tables()
    ehi, elo = split_np(e2)
    fhi, flo = split_np(uf)
    thi, tlo = split_np(uft)
    uhi, ulo = split_np(uh)
    fft = lax.axis_index("x") * 2 + lax.axis_index("yl")
    columns = lax.dynamic_slice_in_dim(col_index, fft * CB, CB)
    k0 = columns // KZ - KZ // 2
    k1 = columns % KZ - KZ // 2
    k2 = jnp.arange(KZ, dtype=jnp.int32) - KZ // 2
    inside = (k0 * k0 + k1 * k1)[None, :] + (k2 * k2)[:, None] <= R2
    masked = jnp.where(inside, coefficients[0], 0.0).reshape(2 * KZ, CB)
    masked = jnp.pad(masked, ((0, 0), (0, 768 - CB)))
    sent = call(
        k1_body,
        "lines",
        smem() + vmem(2),
        shape(ND, R1ROWS, 128),
        [(6, 2 * NZ, 128)],
        10**9,
    )(occupation, masked, fold(w1, 1))
    got = lax.all_to_all(sent, PLANE, split_axis=0, concat_axis=0, tiled=True)
    block = shape(R2ROWS, 128)
    keep2, keep0, keep1, keep3, send2, send_rest = call(
        k2_body,
        "planes",
        [pl.BlockSpec(memory_space=pl.ANY)] + vmem(5),
        (block, block, block, block, block, shape(3, R2ROWS, 128)),
        [
            (48, 48, 128),
            (NCOLS, 128),
            (NCOLS + 56, 128),
            (3, KZ * 24, 128),
            (NP, 2, 4, 40, 256),
            pltpu.SMEM((NCOLS,), jnp.int32),
            pltpu.SemaphoreType.DMA,
        ],
        10**10,
        24,
    )(col_index, got, ehi, elo, fold(er, 1), fold(ug, 2))
    swap = [(0, 1), (1, 0)]
    up = [(i, (i + 1) % 4) for i in range(4)]
    down = [(i, (i - 1) % 4) for i in range(4)]
    keep2 = keep2 + lax.ppermute(send2, "core", swap)
    rest = lax.ppermute(send_rest, "core", swap)
    from_below = lax.ppermute(keep2[:104], "zh", up)
    from_above = lax.ppermute(keep2[104:], "zh", down)
    keep1 = keep1 + rest[1]
    keep3 = keep3 + rest[2]
    keep1 = jnp.concatenate([keep1[:104] + from_below, keep1[104:]], 0)
    keep3 = jnp.concatenate([keep3[:104], keep3[104:] + from_above], 0)
    from_below = lax.ppermute(keep1, "zh", up)
    from_above = lax.ppermute(keep3, "zh", down)
    sent = call(
        k3_body,
        "second",
        vmem(7),
        shape(ND, R3ROWS, 128),
        [(R2ROWS, 128), (184, 128), (3, 184, 128)],
        10**9,
    )(keep0 + rest[0], from_below, from_above, fhi, flo, thi, tlo)
    got = lax.all_to_all(sent, PLANE, split_axis=0, concat_axis=0, tiled=True)
    return call(
        k4_body, "third", vmem(3), shape(9, 36, NF), [(3, NZ, 128), (3, 128, NF)], 10**9
    )(got, uhi, ulo)


def solution(mesh):
    axes = Mesh(mesh.devices.reshape(SIZES), AXES)
    return jax.shard_map(
        local,
        mesh=axes,
        in_specs=(P(BAND, None, None, FFT), P(), P(BAND)),
        out_specs=P(BAND, FFT, None),
        check_vma=False,
    )
```

```python
import jax
import jax.numpy as jnp
import ml_dtypes
import numpy as np
from jax import lax
from jax.experimental import pallas as pl
from jax.experimental.pallas import tpu as pltpu
from jax.sharding import Mesh, PartitionSpec as P

NC = 144
NF = 288
KZ = 72
NCOLS = 5184
BANDS = 32
R2 = (KZ // 2) ** 2

AXES = ("yh", "zh", "zl", "core", "x", "yl")
SIZES = (2, 4, 2, 2, 4, 2)
BAND, FFT = ("yh", "zh", "zl", "core"), ("x", "yl")
PLANE = ("zl", "yh", "yl", "x")
ND = 32
NB = 4
NP = 5
NZ = ND * NP
CB = NCOLS // 8
R1ROWS = 56
R2ROWS = 216
R3ROWS = 16

F32 = jnp.float32
BF16 = jnp.bfloat16


def split_np(table):
    hi = table.astype(np.float32).astype(ml_dtypes.bfloat16)
    lo = (table - hi.astype(np.float64)).astype(np.float32).astype(ml_dtypes.bfloat16)
    return hi, lo


def wave_tables(points):
    k = np.arange(KZ) - KZ // 2
    phase = np.mod(k[:, None] * np.arange(points)[None, :], points) * (2 * np.pi / points)
    return np.cos(phase), np.sin(phase)


def interpolation_np(points):
    offset = np.arange(NF)[:, None] * points - NF * np.arange(points)[None, :]
    k = np.arange(1, NC // 2)
    phase = np.mod(offset[:, :, None] * k, NF * points) * (2 * np.pi / (NF * points))
    return (1 + 2 * np.cos(phase).sum(2)) / points


def tables():
    c, s = wave_tables(NZ)
    w1 = np.concatenate([np.concatenate([c.T, -s.T], 1), np.concatenate([s.T, c.T], 1)], 0)
    c, s = wave_tables(NC)
    e2 = np.zeros((256, 384))
    for ri, (on_re, on_im) in enumerate(((c, -s), (s, c))):
        for at, own in ((128 * ri, slice(0, 128)), (256 + 16 * ri, slice(128, NC))):
            width = own.stop - own.start
            e2[:KZ, at : at + width] = on_re[:, own]
            e2[128 : 128 + KZ, at : at + width] = on_im[:, own]
    er = np.concatenate([np.concatenate([c.T, -s.T], 1), np.concatenate([s.T, c.T], 1)], 0)
    u = interpolation_np(NC)
    ug = np.zeros((2, 4, 40, NC))
    for core in range(2):
        for z in range(8):
            for yh in range(2):
                at = 18 * (z % 2) + 9 * yh
                first = 9 * (16 * yh + 2 * z + core)
                ug[core, z // 2, at : at + 9] = u[first : first + 9]
    ug = ug.reshape(2, 160, NC)
    uf = np.zeros((NC, 384))
    for fb in range(8):
        t, v = divmod(fb, 3)
        uf[:, 128 * t + 36 * v : 128 * t + 36 * v + 36] = u[36 * fb : 36 * fb + 36].T
    uft = np.tile(uf[128:], (8, 1))
    return w1, e2, er, ug, uf[:128], uft, interpolation_np(NZ).T


def fold(table, axis):
    hi, lo = split_np(table)
    return np.concatenate([hi, hi, lo], axis)


def split(x):
    hi = x.astype(BF16)
    return hi, (x - hi.astype(F32)).astype(BF16)


def dot(a, b):
    return jnp.dot(a, b, preferred_element_type=F32)


def dot3(a, b_hi, b_lo):
    hi, lo = split(a)
    return dot(hi, b_hi) + (dot(hi, b_lo) + dot(lo, b_hi))


def lanes(shape):
    return lax.broadcasted_iota(jnp.int32, shape, 1)


def k1_body(occ_ref, x_ref, w_ref, o_ref, ys):
    for n in range(3):
        hi, lo = split(x_ref[:, 256 * n : 256 * n + 256])
        y = dot(w_ref[...], jnp.concatenate([hi, lo, hi], 0))
        ys[2 * n] = y[:, 0:128]
        ys[2 * n + 1] = y[:, 128:256]
    lane = lanes((NZ, 128))
    ys[5, 0:NZ, :] = jnp.where(lane < 8, ys[5, 0:NZ, :], pltpu.roll(ys[5, NZ : 2 * NZ, :], 8, 1))
    weight = jnp.full((1, 128), occ_ref[0].astype(F32) * (1.0 / BANDS), F32)
    for q in range(ND):
        for j in range(6):
            for ri in range(2 if j < 5 else 1):
                at, own = 10 * j + NP * ri, NZ * ri + NP * q
                o_ref[q, at : at + NP, :] = ys[j, own : own + NP, :]
        o_ref[q, 55:56, :] = weight


def rank(yh, fb, zl):
    at = {"yh": yh, "x": fb // 2, "yl": fb % 2, "zl": zl}
    place = 0
    for axis in PLANE:
        place = place * SIZES[AXES.index(axis)] + at[axis]
    return place


def source(b, fb):
    return rank(b // 2, fb, b % 2)


def k2_body(row_ref, r_ref, ehi_ref, elo_ref, er_ref, ug_ref, *rest):
    keep2, keep0, keep1, keep3, send, tr, st, box, hs, gs, col_ref, sem = rest
    columns = pltpu.make_async_copy(row_ref, col_ref, sem)
    columns.start()
    core = lax.axis_index("core")
    zh = lax.axis_index("zh")
    box[NCOLS : NCOLS + 56, :] = jnp.zeros((56, 128), F32)

    def unpack(fb, carry):
        base = fb * CB
        for j in range(6):
            for b in range(NB):
                for ri in range(2 if j < 5 else 1):
                    at = 24 * ri + NP * b
                    own = 10 * j + NP * ri
                    tr[6 * fb + j, at : at + NP, :] = r_ref[source(b, fb), own : own + NP, :]
            if j < 5:
                st[pl.ds(base + 128 * j, 128), 0:48] = tr[6 * fb + j].T
            else:
                tr[6 * fb + 5, 24:48, :] = pltpu.roll(tr[6 * fb + 5, 0:24, :], 120, 1)
                st[pl.ds(base + 640, 8), 0:48] = tr[6 * fb + 5].T[0:8]
        return carry

    for fb in range(8):
        unpack(fb, 0)
    columns.wait()

    views = [col_ref.at[pl.ds(t, NCOLS - 432 + 1)] for t in range(432)]

    def place(i, carry):
        at = i * 432
        for t in range(432):
            box[pl.ds(views[t][at], 1), :] = st[pl.ds(at + t, 1), :]
        return carry

    lax.fori_loop(0, NCOLS // 432, place, 0)

    def along_second(i, carry):
        parts = []
        for t in range(36):
            at = pl.multiple_of((i * 36 + t) * KZ, 8)
            flipped = box[pl.ds(at, 128), :].T
            parts.append(jnp.concatenate([flipped[0:24], flipped[24:48]], 1))
        line = jnp.concatenate(parts, 0)
        half = dot3(line, ehi_ref[...], elo_ref[...])
        for j in range(3):
            hs[j, pl.ds(pl.multiple_of(i * 864, 8), 864), :] = half[:, 128 * j : 128 * j + 128]
        return carry

    lax.fori_loop(0, 2, along_second, 0)

    lane = lanes((NC, 128))

    def transformed(field):
        hi, lo = split(field)
        full = dot(er_ref[...], jnp.concatenate([hi, lo, hi], 0))
        sq = full * full
        return sq[0:NC] + sq[NC : 2 * NC]

    def plane(p, carry):
        weight = [r_ref[source(b, 0), 55:56, 0:1] for b in range(NB)]
        mains, tail, factor = [], None, None
        for b in range(NB):
            re, im, end = [hs[j, pl.ds(NP * b + p, KZ, stride=24), :] for j in range(3)]
            mains.append(jnp.concatenate([re, im], 0))
            re = pltpu.roll(end, 16 * b, 1) if b else end
            im = pltpu.roll(end, 16 * b - 16, 1) if b > 1 else end if b else pltpu.roll(end, 112, 1)
            end = jnp.concatenate([re, im], 0)
            tail = jnp.where(lane < 16 * b, tail, end) if b else end
            factor = jnp.where(lane < 16 * b, factor, weight[b]) if b else weight[b]
        density = None
        for b in range(0, NB, 2):
            pair = transformed(jnp.concatenate(mains[b : b + 2], 1))
            pair = pair[:, 0:128] * weight[b] + pair[:, 128:256] * weight[b + 1]
            density = pair if density is None else density + pair
        tail = transformed(tail) * factor
        tail = tail + pltpu.roll(tail, 96, 1)
        tail = tail + pltpu.roll(tail, 112, 1)
        density = jnp.concatenate([density, tail], 1)
        hi, lo = split(density)
        rhs = jnp.concatenate([hi, lo, hi], 0)
        gs[p, 0] = dot(ug_ref[core], rhs).reshape(4, 40, 256)
        gs[p, 1] = dot(ug_ref[1 - core], rhs).reshape(4, 40, 256)
        return carry

    for p in range(NP):
        plane(p, 0)
    tail_lane = lanes((36, 128))
    sends = [send.at[d] for d in range(4)]
    for part, outs in enumerate(((keep0, keep1, keep2, keep3), sends)):
        for d in range(4):
            z = (zh + d) & 3
            tail = None
            for p in range(NP):
                outs[d][36 * p : 36 * p + 36, :] = gs[p, part, z, 0:36, 0:128]
                end = gs[p, part, z, 0:36, 128:256]
                if p == 0:
                    tail = end
                else:
                    tail = jnp.where(tail_lane < 16 * p, tail, pltpu.roll(end, 16 * p, 1))
            outs[d][36 * NP : 36 * NP + 36, :] = tail


def k3_body(r0_ref, r1_ref, r2_ref, fhi_ref, flo_ref, thi_ref, tlo_ref, o_ref, ss, ts, fs):
    ss[...] = r0_ref[...] + (r1_ref[...] + r2_ref[...])
    lane = lanes((36, 128))
    ts[176:184, :] = jnp.zeros((8, 128), F32)
    for p in range(NP):
        own = (lane >= 16 * p) & (lane < 16 * p + 16)
        ts[36 * p : 36 * p + 36, :] = jnp.where(own, ss[36 * NP : 36 * NP + 36, :], 0.0)
    fine = dot3(ss[0:184, :], fhi_ref[...], flo_ref[...]) + dot3(
        ts[...], thi_ref[...], tlo_ref[...]
    )
    for t in range(3):
        fs[t] = fine[:, 128 * t : 128 * t + 128]
    lane = lanes((NP, 128))
    for yh in range(2):
        for zl in range(2):
            for fb in range(8):
                t, v = divmod(fb, 3)
                for b in range(3):
                    acc = None
                    for a in range(3):
                        first = 18 * zl + 9 * yh + 3 * a + b
                        part = fs[t, pl.ds(first, NP, stride=36), :]
                        if a != v:
                            part = pltpu.roll(part, (36 * (a - v)) % 128, 1)
                        acc = part if acc is None else jnp.where(lane < 36 * a, acc, part)
                    o_ref[rank(yh, fb, zl), NP * b : NP * b + NP, :] = acc


def k4_body(r_ref, uhi_ref, ulo_ref, o_ref, xs, ys):
    for b in range(3):
        for q in range(ND):
            xs[b, NP * q : NP * q + NP, :] = r_ref[q, NP * b : NP * b + NP, :]
        ys[b] = dot3(xs[b].T, uhi_ref[...], ulo_ref[...])
        for a in range(3):
            o_ref[3 * a + b] = ys[b, 36 * a : 36 * a + 36, :]


def vmem(n):
    return [pl.BlockSpec(memory_space=pltpu.VMEM)] * n


def smem():
    return [pl.BlockSpec(memory_space=pltpu.SMEM)]


def call(body, name, in_specs, outs, scratch, flops, mib=12):
    return pl.pallas_call(
        body,
        out_shape=outs,
        in_specs=in_specs,
        out_specs=jax.tree.map(lambda _: pl.BlockSpec(memory_space=pltpu.VMEM), outs),
        scratch_shapes=[pltpu.VMEM(s, F32) if isinstance(s, tuple) else s for s in scratch],
        name=name,
        compiler_params=pltpu.CompilerParams(vmem_limit_bytes=mib * 2**20),
        cost_estimate=pl.CostEstimate(flops=flops, bytes_accessed=2_000_000, transcendentals=0),
    )


def shape(*dims):
    return jax.ShapeDtypeStruct(dims, F32)


def local(coefficients, col_index, occupation):
    w1, e2, er, ug, uf, uft, uh = tables()
    ehi, elo = split_np(e2)
    fhi, flo = split_np(uf)
    thi, tlo = split_np(uft)
    uhi, ulo = split_np(uh)
    fft = lax.axis_index("x") * 2 + lax.axis_index("yl")
    columns = lax.dynamic_slice_in_dim(col_index, fft * CB, CB)
    k0 = columns // KZ - KZ // 2
    k1 = columns % KZ - KZ // 2
    k2 = jnp.arange(KZ, dtype=jnp.int32) - KZ // 2
    inside = (k0 * k0 + k1 * k1)[None, :] + (k2 * k2)[:, None] <= R2
    masked = jnp.where(inside, coefficients[0], 0.0).reshape(2 * KZ, CB)
    masked = jnp.pad(masked, ((0, 0), (0, 768 - CB)))
    sent = call(
        k1_body,
        "lines",
        smem() + vmem(2),
        shape(ND, R1ROWS, 128),
        [(6, 2 * NZ, 128)],
        10**9,
    )(occupation, masked, fold(w1, 1))
    got = lax.all_to_all(sent, PLANE, split_axis=0, concat_axis=0, tiled=True)
    block = shape(R2ROWS, 128)
    keep2, keep0, keep1, keep3, send = call(
        k2_body,
        "planes",
        [pl.BlockSpec(memory_space=pl.ANY)] + vmem(5),
        (block, block, block, block, shape(4, R2ROWS, 128)),
        [
            (48, 48, 128),
            (NCOLS, 128),
            (NCOLS + 56, 128),
            (3, KZ * 24, 128),
            (NP, 2, 4, 40, 256),
            pltpu.SMEM((NCOLS,), jnp.int32),
            pltpu.SemaphoreType.DMA,
        ],
        10**10,
        24,
    )(col_index, got, ehi, elo, fold(er, 1), fold(ug, 2))
    swap = [(0, 1), (1, 0)]
    up = [(i, (i + 1) % 4) for i in range(4)]
    down = [(i, (i - 1) % 4) for i in range(4)]
    swapped = lax.ppermute(send, "core", swap)
    keep2 = keep2 + swapped[2]
    from_below = lax.ppermute(keep2[:104], "zh", up)
    from_above = lax.ppermute(keep2[104:], "zh", down)
    keep1 = keep1 + swapped[1]
    keep3 = keep3 + swapped[3]
    keep1 = jnp.concatenate([keep1[:104] + from_below, keep1[104:]], 0)
    keep3 = jnp.concatenate([keep3[:104], keep3[104:] + from_above], 0)
    from_below = lax.ppermute(keep1, "zh", up)
    from_above = lax.ppermute(keep3, "zh", down)
    sent = call(
        k3_body,
        "second",
        vmem(7),
        shape(ND, R3ROWS, 128),
        [(R2ROWS, 128), (184, 128), (3, 184, 128)],
        10**9,
    )(keep0 + swapped[0], from_below, from_above, fhi, flo, thi, tlo)
    got = lax.all_to_all(sent, PLANE, split_axis=0, concat_axis=0, tiled=True)
    return call(
        k4_body, "third", vmem(3), shape(9, 36, NF), [(3, NZ, 128), (3, 128, NF)], 10**9
    )(got, uhi, ulo)


def solution(mesh):
    axes = Mesh(mesh.devices.reshape(SIZES), AXES)
    return jax.shard_map(
        local,
        mesh=axes,
        in_specs=(P(BAND, None, None, FFT), P(), P(BAND)),
        out_specs=P(BAND, FFT, None),
        check_vma=False,
    )
```

```python
import jax
import jax.numpy as jnp
import ml_dtypes
import numpy as np
from jax import lax
from jax.experimental import pallas as pl
from jax.experimental.pallas import tpu as pltpu
from jax.sharding import Mesh, PartitionSpec as P

NC = 144
NF = 288
KZ = 72
NCOLS = 5184
BANDS = 32
R2 = (KZ // 2) ** 2

AXES = ("yh", "zh", "zl", "core", "x", "yl")
SIZES = (2, 4, 2, 2, 4, 2)
BAND, FFT = ("yh", "zh", "zl", "core"), ("x", "yl")
PLANE = ("yh", "x", "yl", "zl")
ND = 32
NB = 4
NP = 5
NZ = ND * NP
CB = NCOLS // 8
R1ROWS = 56
R2ROWS = 216
R3ROWS = 16

F32 = jnp.float32
BF16 = jnp.bfloat16


def split_np(table):
    hi = table.astype(np.float32).astype(ml_dtypes.bfloat16)
    lo = (table - hi.astype(np.float64)).astype(np.float32).astype(ml_dtypes.bfloat16)
    return hi, lo


def wave_tables(points):
    k = np.arange(KZ) - KZ // 2
    phase = np.mod(k[:, None] * np.arange(points)[None, :], points) * (2 * np.pi / points)
    return np.cos(phase), np.sin(phase)


def interpolation_np(points):
    offset = np.arange(NF)[:, None] * points - NF * np.arange(points)[None, :]
    k = np.arange(1, NC // 2)
    phase = np.mod(offset[:, :, None] * k, NF * points) * (2 * np.pi / (NF * points))
    return (1 + 2 * np.cos(phase).sum(2)) / points


def tables():
    c, s = wave_tables(NZ)
    w1 = np.concatenate([np.concatenate([c.T, -s.T], 1), np.concatenate([s.T, c.T], 1)], 0)
    c, s = wave_tables(NC)
    e2 = np.zeros((256, 384))
    for ri, (on_re, on_im) in enumerate(((c, -s), (s, c))):
        for at, own in ((128 * ri, slice(0, 128)), (256 + 16 * ri, slice(128, NC))):
            width = own.stop - own.start
            e2[:KZ, at : at + width] = on_re[:, own]
            e2[128 : 128 + KZ, at : at + width] = on_im[:, own]
    er = np.concatenate([np.concatenate([c.T, -s.T], 1), np.concatenate([s.T, c.T], 1)], 0)
    u = interpolation_np(NC)
    ug = np.zeros((2, 4, 40, NC))
    for core in range(2):
        for z in range(8):
            for yh in range(2):
                at = 18 * (z % 2) + 9 * yh
                first = 9 * (16 * yh + 2 * z + core)
                ug[core, z // 2, at : at + 9] = u[first : first + 9]
    ug = ug.reshape(2, 160, NC)
    uf = np.zeros((NC, 384))
    for fb in range(8):
        t, v = divmod(fb, 3)
        uf[:, 128 * t + 36 * v : 128 * t + 36 * v + 36] = u[36 * fb : 36 * fb + 36].T
    uft = np.tile(uf[128:], (8, 1))
    return w1, e2, er, ug, uf[:128], uft, interpolation_np(NZ).T


def fold(table, axis):
    hi, lo = split_np(table)
    return np.concatenate([hi, hi, lo], axis)


def split(x):
    hi = x.astype(BF16)
    return hi, (x - hi.astype(F32)).astype(BF16)


def dot(a, b):
    return jnp.dot(a, b, preferred_element_type=F32)


def dot3(a, b_hi, b_lo):
    hi, lo = split(a)
    return dot(hi, b_hi) + (dot(hi, b_lo) + dot(lo, b_hi))


def lanes(shape):
    return lax.broadcasted_iota(jnp.int32, shape, 1)


def k1_body(occ_ref, x_ref, w_ref, o_ref, ys):
    for n in range(3):
        hi, lo = split(x_ref[:, 256 * n : 256 * n + 256])
        y = dot(w_ref[...], jnp.concatenate([hi, lo, hi], 0))
        ys[2 * n] = y[:, 0:128]
        ys[2 * n + 1] = y[:, 128:256]
    lane = lanes((NZ, 128))
    ys[5, 0:NZ, :] = jnp.where(lane < 8, ys[5, 0:NZ, :], pltpu.roll(ys[5, NZ : 2 * NZ, :], 8, 1))
    weight = jnp.full((1, 128), occ_ref[0].astype(F32) * (1.0 / BANDS), F32)
    for q in range(ND):
        for j in range(6):
            for ri in range(2 if j < 5 else 1):
                at, own = 10 * j + NP * ri, NZ * ri + NP * q
                o_ref[q, at : at + NP, :] = ys[j, own : own + NP, :]
        o_ref[q, 55:56, :] = weight


def source(b, fb):
    return 16 * (b // 2) + 2 * fb + b % 2


def k2_body(row_ref, r_ref, ehi_ref, elo_ref, er_ref, ug_ref, *rest):
    keep2, keep0, keep1, keep3, send, tr, st, box, hs, gs, col_ref, sem = rest
    columns = pltpu.make_async_copy(row_ref, col_ref, sem)
    columns.start()
    core = lax.axis_index("core")
    zh = lax.axis_index("zh")
    box[NCOLS : NCOLS + 56, :] = jnp.zeros((56, 128), F32)

    def unpack(fb, carry):
        base = fb * CB
        for j in range(6):
            for b in range(NB):
                for ri in range(2 if j < 5 else 1):
                    at = 24 * ri + NP * b
                    own = 10 * j + NP * ri
                    tr[6 * fb + j, at : at + NP, :] = r_ref[source(b, fb), own : own + NP, :]
            if j < 5:
                st[pl.ds(base + 128 * j, 128), 0:48] = tr[6 * fb + j].T
            else:
                tr[6 * fb + 5, 24:48, :] = pltpu.roll(tr[6 * fb + 5, 0:24, :], 120, 1)
                st[pl.ds(base + 640, 8), 0:48] = tr[6 * fb + 5].T[0:8]
        return carry

    for fb in range(8):
        unpack(fb, 0)
    columns.wait()

    views = [col_ref.at[pl.ds(t, NCOLS - 432 + 1)] for t in range(432)]

    def place(i, carry):
        at = i * 432
        for t in range(432):
            box[pl.ds(views[t][at], 1), :] = st[pl.ds(at + t, 1), :]
        return carry

    lax.fori_loop(0, NCOLS // 432, place, 0)

    def along_second(i, carry):
        parts = []
        for t in range(72):
            at = (i * 72 + t) * KZ
            flipped = box[pl.ds(at, 128), :].T
            parts.append(jnp.concatenate([flipped[0:24], flipped[24:48]], 1))
        line = jnp.concatenate(parts, 0)
        half = dot3(line, ehi_ref[...], elo_ref[...])
        for j in range(3):
            hs[j, pl.ds(i * 1728, 1728), :] = half[:, 128 * j : 128 * j + 128]
        return carry

    along_second(0, 0)

    lane = lanes((NC, 128))

    def transformed(field):
        hi, lo = split(field)
        full = dot(er_ref[...], jnp.concatenate([hi, lo, hi], 0))
        sq = full * full
        return sq[0:NC] + sq[NC : 2 * NC]

    def plane(p, carry):
        weight = [r_ref[source(b, 0), 55:56, 0:1] for b in range(NB)]
        mains, tail, factor = [], None, None
        for b in range(NB):
            re, im, end = [hs[j, pl.ds(NP * b + p, KZ, stride=24), :] for j in range(3)]
            mains.append(jnp.concatenate([re, im], 0))
            re = pltpu.roll(end, 16 * b, 1) if b else end
            im = pltpu.roll(end, 16 * b - 16, 1) if b > 1 else end if b else pltpu.roll(end, 112, 1)
            end = jnp.concatenate([re, im], 0)
            tail = jnp.where(lane < 16 * b, tail, end) if b else end
            factor = jnp.where(lane < 16 * b, factor, weight[b]) if b else weight[b]
        density = None
        for b in range(0, NB, 2):
            pair = transformed(jnp.concatenate(mains[b : b + 2], 1))
            pair = pair[:, 0:128] * weight[b] + pair[:, 128:256] * weight[b + 1]
            density = pair if density is None else density + pair
        tail = transformed(tail) * factor
        tail = tail + pltpu.roll(tail, 96, 1)
        tail = tail + pltpu.roll(tail, 112, 1)
        density = jnp.concatenate([density, tail], 1)
        hi, lo = split(density)
        rhs = jnp.concatenate([hi, lo, hi], 0)
        gs[p, 0] = dot(ug_ref[core], rhs).reshape(4, 40, 256)
        gs[p, 1] = dot(ug_ref[1 - core], rhs).reshape(4, 40, 256)
        return carry

    for p in range(NP):
        plane(p, 0)
    tail_lane = lanes((36, 128))
    sends = [send.at[d] for d in range(4)]
    for part, outs in enumerate(((keep0, keep1, keep2, keep3), sends)):
        for d in range(4):
            z = (zh + d) & 3
            tail = None
            for p in range(NP):
                outs[d][36 * p : 36 * p + 36, :] = gs[p, part, z, 0:36, 0:128]
                end = gs[p, part, z, 0:36, 128:256]
                if p == 0:
                    tail = end
                else:
                    tail = jnp.where(tail_lane < 16 * p, tail, pltpu.roll(end, 16 * p, 1))
            outs[d][36 * NP : 36 * NP + 36, :] = tail


def k3_body(r0_ref, r1_ref, r2_ref, fhi_ref, flo_ref, thi_ref, tlo_ref, o_ref, ss, ts, fs):
    ss[...] = r0_ref[...] + (r1_ref[...] + r2_ref[...])
    lane = lanes((36, 128))
    ts[176:184, :] = jnp.zeros((8, 128), F32)
    for p in range(NP):
        own = (lane >= 16 * p) & (lane < 16 * p + 16)
        ts[36 * p : 36 * p + 36, :] = jnp.where(own, ss[36 * NP : 36 * NP + 36, :], 0.0)
    fine = dot3(ss[0:184, :], fhi_ref[...], flo_ref[...]) + dot3(
        ts[...], thi_ref[...], tlo_ref[...]
    )
    for t in range(3):
        fs[t] = fine[:, 128 * t : 128 * t + 128]
    lane = lanes((NP, 128))
    for yh in range(2):
        for zl in range(2):
            for fb in range(8):
                t, v = divmod(fb, 3)
                for b in range(3):
                    acc = None
                    for a in range(3):
                        first = 18 * zl + 9 * yh + 3 * a + b
                        part = fs[t, pl.ds(first, NP, stride=36), :]
                        if a != v:
                            part = pltpu.roll(part, (36 * (a - v)) % 128, 1)
                        acc = part if acc is None else jnp.where(lane < 36 * a, acc, part)
                    o_ref[16 * yh + 2 * fb + zl, NP * b : NP * b + NP, :] = acc


def k4_body(r_ref, uhi_ref, ulo_ref, o_ref, xs, ys):
    for b in range(3):
        for q in range(ND):
            xs[b, NP * q : NP * q + NP, :] = r_ref[q, NP * b : NP * b + NP, :]
        ys[b] = dot3(xs[b].T, uhi_ref[...], ulo_ref[...])
        for a in range(3):
            o_ref[3 * a + b] = ys[b, 36 * a : 36 * a + 36, :]


def vmem(n):
    return [pl.BlockSpec(memory_space=pltpu.VMEM)] * n


def smem():
    return [pl.BlockSpec(memory_space=pltpu.SMEM)]


def call(body, name, in_specs, outs, scratch, flops, mib=12):
    return pl.pallas_call(
        body,
        out_shape=outs,
        in_specs=in_specs,
        out_specs=jax.tree.map(lambda _: pl.BlockSpec(memory_space=pltpu.VMEM), outs),
        scratch_shapes=[pltpu.VMEM(s, F32) if isinstance(s, tuple) else s for s in scratch],
        name=name,
        compiler_params=pltpu.CompilerParams(vmem_limit_bytes=mib * 2**20),
        cost_estimate=pl.CostEstimate(flops=flops, bytes_accessed=2_000_000, transcendentals=0),
    )


def shape(*dims):
    return jax.ShapeDtypeStruct(dims, F32)


def local(coefficients, col_index, occupation):
    w1, e2, er, ug, uf, uft, uh = tables()
    ehi, elo = split_np(e2)
    fhi, flo = split_np(uf)
    thi, tlo = split_np(uft)
    uhi, ulo = split_np(uh)
    fft = lax.axis_index("x") * 2 + lax.axis_index("yl")
    columns = lax.dynamic_slice_in_dim(col_index, fft * CB, CB)
    k0 = columns // KZ - KZ // 2
    k1 = columns % KZ - KZ // 2
    k2 = jnp.arange(KZ, dtype=jnp.int32) - KZ // 2
    inside = (k0 * k0 + k1 * k1)[None, :] + (k2 * k2)[:, None] <= R2
    masked = jnp.where(inside, coefficients[0], 0.0).reshape(2 * KZ, CB)
    masked = jnp.pad(masked, ((0, 0), (0, 768 - CB)))
    sent = call(
        k1_body,
        "lines",
        smem() + vmem(2),
        shape(ND, R1ROWS, 128),
        [(6, 2 * NZ, 128)],
        10**9,
    )(occupation, masked, fold(w1, 1))
    got = lax.all_to_all(sent, PLANE, split_axis=0, concat_axis=0, tiled=True)
    block = shape(R2ROWS, 128)
    keep2, keep0, keep1, keep3, send = call(
        k2_body,
        "planes",
        [pl.BlockSpec(memory_space=pl.ANY)] + vmem(5),
        (block, block, block, block, shape(4, R2ROWS, 128)),
        [
            (48, 48, 128),
            (NCOLS, 128),
            (NCOLS + 56, 128),
            (3, KZ * 24, 128),
            (NP, 2, 4, 40, 256),
            pltpu.SMEM((NCOLS,), jnp.int32),
            pltpu.SemaphoreType.DMA,
        ],
        10**10,
        32,
    )(col_index, got, ehi, elo, fold(er, 1), fold(ug, 2))
    swap = [(0, 1), (1, 0)]
    up = [(i, (i + 1) % 4) for i in range(4)]
    down = [(i, (i - 1) % 4) for i in range(4)]
    swapped = lax.ppermute(send, "core", swap)
    keep2 = keep2 + swapped[2]
    from_below = lax.ppermute(keep2[:104], "zh", up)
    from_above = lax.ppermute(keep2[104:], "zh", down)
    keep1 = keep1 + swapped[1]
    keep3 = keep3 + swapped[3]
    keep1 = jnp.concatenate([keep1[:104] + from_below, keep1[104:]], 0)
    keep3 = jnp.concatenate([keep3[:104], keep3[104:] + from_above], 0)
    from_below = lax.ppermute(keep1, "zh", up)
    from_above = lax.ppermute(keep3, "zh", down)
    sent = call(
        k3_body,
        "second",
        vmem(7),
        shape(ND, R3ROWS, 128),
        [(R2ROWS, 128), (184, 128), (3, 184, 128)],
        10**9,
    )(keep0 + swapped[0], from_below, from_above, fhi, flo, thi, tlo)
    got = lax.all_to_all(sent, PLANE, split_axis=0, concat_axis=0, tiled=True)
    return call(
        k4_body, "third", vmem(3), shape(9, 36, NF), [(3, NZ, 128), (3, 128, NF)], 10**9
    )(got, uhi, ulo)


def solution(mesh):
    axes = Mesh(mesh.devices.reshape(SIZES), AXES)
    return jax.shard_map(
        local,
        mesh=axes,
        in_specs=(P(BAND, None, None, FFT), P(), P(BAND)),
        out_specs=P(BAND, FFT, None),
        check_vma=False,
    )
```
